128 devices in a mesh: batch: 1, cols: 64 (over z, y, x), rows: 2 (over core).
Axes of the slice: x: 4, y: 4, z: 4, core: 2. Of those that a mesh axis runs over, the one named last changes fastest.
Arguments:
- frames: bfloat16 [4, 16, 16, 512, 384], P(None, 'batch', 'rows', 'cols')
- h_init: float32 [16, 16, 512, 384], P('batch', 'rows', 'cols')
- w_x: bfloat16 [3, 3, 384, 1152], replicated
- w_hzr: bfloat16 [3, 3, 384, 768], replicated
- w_hn: bfloat16 [3, 3, 384, 384], replicated
- gate_bias: float32 [1152], replicated
Outputs:
- output 1: bfloat16 [4, 16, 16, 512, 384], P(None, 'batch', 'rows', 'cols')
- output 2: float32 [16, 16, 512, 384], P('batch', 'rows', 'cols')
All inputs are finite; a program needn't handle non-finite values.
Results may differ from the reference program's by a relative error of at most 0.00190342.
Values are sent between devices in bfloat16 or wider.
A program may use at most 1 GiB of HBM per device.

```python
import jax
import jax.numpy as jnp
from jax import lax

STEPS = 4
BATCH = 16
HEIGHT = 16
WIDTH = 512
CIN = 384
CH = 384


def setup_inputs(seed: int = 0, part: int = 0) -> dict:
    keys = jax.random.split(jax.random.key(seed), 6)
    key_frames = jax.random.fold_in(keys[0], part)
    key_state = jax.random.fold_in(keys[1], part)
    frames = jax.random.normal(key_frames, (STEPS, BATCH, HEIGHT, WIDTH, CIN), jnp.float32).astype(jnp.bfloat16)
    h_init = 0.8 * jax.random.normal(key_state, (BATCH, HEIGHT, WIDTH, CH), jnp.float32)
    w_x = (jax.random.normal(keys[2], (3, 3, CIN, 3 * CH), jnp.float32) * (9 * CIN) ** -0.5).astype(jnp.bfloat16)
    w_hzr = (jax.random.normal(keys[3], (3, 3, CH, 2 * CH), jnp.float32) * (1.5 * (9 * CH) ** -0.5)).astype(jnp.bfloat16)
    w_hn = (jax.random.normal(keys[4], (3, 3, CH, CH), jnp.float32) * (2.0 * (9 * CH) ** -0.5)).astype(jnp.bfloat16)
    gate_bias = 0.5 * jax.random.normal(keys[5], (3 * CH,), jnp.float32)
    return {'frames': frames, 'h_init': h_init, 'w_x': w_x, 'w_hzr': w_hzr, 'w_hn': w_hn, 'gate_bias': gate_bias}


def conv_same(inputs, weights):
    return lax.conv_general_dilated(inputs.astype(jnp.float32), weights.astype(jnp.float32), (1, 1), 'SAME', dimension_numbers=('NHWC', 'HWIO', 'NHWC'), precision=lax.Precision.HIGHEST)


def reference(frames, h_init, w_x, w_hzr, w_hn, gate_bias):
    def one_step(h_prev, frame_t):
        gate_x = conv_same(frame_t, w_x) + gate_bias
        zr_gates = jax.nn.sigmoid(gate_x[..., :2 * CH] + conv_same(h_prev.astype(jnp.bfloat16), w_hzr))
        update = zr_gates[..., :CH]
        reset_hid = (zr_gates[..., CH:] * h_prev).astype(jnp.bfloat16)
        candidate = jnp.tanh(gate_x[..., 2 * CH:] + conv_same(reset_hid, w_hn))
        h_next = (1.0 - update) * candidate + update * h_prev
        return h_next, h_next.astype(jnp.bfloat16)
    h_last, h_seq = lax.scan(one_step, h_init, frames)
    return h_seq, h_last
```

```python
import jax
import jax.numpy as jnp
from jax import lax
from jax.experimental import pallas as pl
from jax.experimental.pallas import tpu as pltpu
from jax.sharding import PartitionSpec as P

MESH = pl.DeviceIdType.MESH
BF = jnp.bfloat16
F32 = jnp.float32
L = 128


def sigmoid(v):
    return 0.5 * jnp.tanh(0.5 * v) + 0.5


def make_kernel(steps, tile_h, tile_w, batch, ch, n_cols):
    half_w = tile_w // 2

    def kernel(frames, h0, wx, wz, wn, bias, h_seq, h_last,
               xb, hb, rb, hf, zf, gv, wxv, wzv, wnv, send_sem, recv_sem, load_sem, out_sem):
        row = lax.axis_index('rows')
        col = lax.axis_index('cols')
        has_left = col > 0
        has_right = col < n_cols - 1
        left, right, other = col - 1, col + 1, 1 - row
        src_row = tile_h - (tile_h - 1) * row
        dst_row = (tile_h + 1) * row

        inner = (pl.ds(1, tile_h), pl.ds(1, tile_w))

        def load_frame(t):
            return pltpu.make_async_copy(frames.at[t], xb.at[(t,) + inner], load_sem.at[t])

        def load_w(src, dst, first, width, sem):
            return pltpu.make_async_copy(src.at[:, pl.ds(first, width)], dst.at[:, pl.ds(first, width)], load_sem.at[sem])

        load_h = pltpu.make_async_copy(h0, hf, load_sem.at[steps])
        s0 = steps + 1
        load_xa = load_w(wx, wxv, 0, 256, s0)
        load_xd = load_w(wx, wxv, 768, 256, s0 + 1)
        load_xbc = load_w(wx, wxv, 256, 512, s0 + 2)
        load_z = load_w(wz, wzv, 0, 768, s0 + 3)
        load_xe = load_w(wx, wxv, 1024, 128, s0 + 4)
        load_n = load_w(wn, wnv, 0, 384, s0 + 5)
        load_frame(0).start()
        load_xa.start()
        load_h.start()
        load_xd.start()
        load_xbc.start()
        load_z.start()
        load_xe.start()
        load_n.start()
        for t in range(1, steps):
            load_frame(t).start()

        def zero_border(buf, i):
            edge = jnp.zeros((tile_w + 2, batch, ch), BF)
            buf[i, 0] = edge
            buf[i, tile_h + 1] = edge
            side = jnp.zeros((tile_h, 1, batch, ch), BF)
            buf[i, 1:tile_h + 1, 0:1] = side
            buf[i, 1:tile_h + 1, tile_w + 1:tile_w + 2] = side

        for i in range(2):
            zero_border(hb, i)
            zero_border(rb, i)

        @pl.loop(0, steps)
        def _(t):
            zero_border(xb, t)

        barrier = pltpu.get_barrier_semaphore()

        def greet(c, r):
            pl.semaphore_signal(barrier, inc=1, device_id={'cols': c, 'rows': r}, device_id_type=MESH)

        greet(col, other)

        @pl.when(has_left)
        def _():
            greet(left, row)
            greet(left, other)

        @pl.when(has_right)
        def _():
            greet(right, row)
            greet(right, other)

        pl.semaphore_wait(barrier, 1 + 2 * jnp.minimum(col, 1) + 2 * jnp.minimum(n_cols - 1 - col, 1))

        def copies(buf, i, slot):
            def rc(src, dst, k, c, r):
                return pltpu.make_async_remote_copy(
                    src_ref=buf.at[(i,) + src], dst_ref=buf.at[(i,) + dst], send_sem=send_sem.at[slot, k],
                    recv_sem=recv_sem.at[slot, k], device_id={'cols': c, 'rows': r}, device_id_type=MESH)
            rows = pl.ds(1, tile_h)
            return (
                rc((src_row, pl.ds(1, tile_w)), (dst_row, pl.ds(1, tile_w)), 0, col, other),
                rc((rows, 1), (rows, tile_w + 1), 1, left, row),
                rc((rows, tile_w), (rows, 0), 2, right, row),
                rc((src_row, 1), (dst_row, tile_w + 1), 3, left, other),
                rc((src_row, tile_w), (dst_row, 0), 4, right, other),
            )

        def send(buf, i, slot):
            cp = copies(buf, i, slot)
            cp[0].start()

            @pl.when(has_left)
            def _():
                cp[1].start()
                cp[3].start()

            @pl.when(has_right)
            def _():
                cp[2].start()
                cp[4].start()

        def wait_rows(buf, i, slot):
            copies(buf, i, slot)[0].wait_recv()

        def wait_cols(buf, i, slot):
            cp = copies(buf, i, slot)
            cp[0].wait_send()

            @pl.when(has_left)
            def _():
                cp[2].wait_recv()
                cp[4].wait_recv()
                cp[1].wait_send()
                cp[3].wait_send()

            @pl.when(has_right)
            def _():
                cp[1].wait_recv()
                cp[3].wait_recv()
                cp[2].wait_send()
                cp[4].wait_send()

        half_m = tile_h * half_w * batch

        def taps(buf, i, w, first, n, q, which):
            lhs, rhs = [], []
            for c in which[q]:
                for a in range(3):
                    lhs.append(buf[i, a:a + tile_h, q * half_w + c:q * half_w + c + half_w].reshape(half_m, ch))
                    rhs.append(w[(a * 3 + c) * ch:(a * 3 + c + 1) * ch, first:first + n])
            return lhs, rhs

        near6 = ((1, 2), (1, 0))
        far3 = ((0,), (2,))

        def product(lhs, rhs):
            return jnp.dot(jnp.concatenate(lhs, axis=1), jnp.concatenate(rhs, axis=0),
                           preferred_element_type=F32).reshape(tile_h, half_w, batch, -1)

        def six(buf, i, w, first, n=256):
            return [product(*taps(buf, i, w, first, n, q, near6)) for q in range(2)]

        def last(t, first_x, buf, i, w, first, n=256):
            out = []
            for q in range(2):
                lx, rx = taps(xb, t, wxv, first_x, n, q, far3)
                lh, rh = taps(buf, i, w, first, n, q, far3)
                out.append(product(lx + lh, rx + rh))
            return out

        def at(q):
            return (slice(None), slice(q * half_w, (q + 1) * half_w))

        def at_pad(q):
            return (slice(1, tile_h + 1), slice(1 + q * half_w, 1 + (q + 1) * half_w))

        def put(s, vals):
            for q in range(2):
                n = vals[q].shape[-1]
                gv[(s,) + at(q) + (slice(None), slice(0, n))] = vals[q]

        def add(s, vals):
            for q in range(2):
                n = vals[q].shape[-1]
                idx = (s,) + at(q) + (slice(None), slice(0, n))
                gv[idx] = gv[idx] + vals[q]

        def total(s, vals):
            return [vals[q] + gv[(s,) + at(q) + (slice(None), slice(0, vals[q].shape[-1]))] for q in range(2)]

        def lanes(g):
            return (slice(None), slice(g * L, (g + 1) * L))

        def b_of(first):
            return bias[0:1, first:first + L].reshape(1, 1, 1, L)

        def reset_part(v, g, q, par):
            r = sigmoid(v + b_of(ch + g * L))
            rb[(par,) + at_pad(q) + lanes(g)] = (r * hf[at(q) + lanes(g)]).astype(BF)

        def update_part(v, g, q):
            zf[at(q) + lanes(g)] = sigmoid(v + b_of(g * L))

        def state_part(v, g, q, nxt):
            idx = at(q) + lanes(g)
            n = jnp.tanh(v + b_of(2 * ch + g * L))
            z = zf[idx]
            h = (1.0 - z) * n + z * hf[idx]
            hf[idx] = h
            hb[(nxt,) + at_pad(q) + lanes(g)] = h.astype(BF)

        def store_step(t, nxt):
            return pltpu.make_async_copy(hb.at[(nxt,) + inner], h_seq.at[t], out_sem.at[nxt])

        h_slot, r_slot = steps, steps + 2

        load_frame(0).wait()
        send(xb, 0, 0)
        load_h.wait()

        @pl.loop(0, tile_h)
        def _(r):
            hb[0, 1 + r, 1:tile_w + 1] = hf[r].astype(BF)

        send(hb, 0, h_slot)
        load_xa.wait()
        wait_rows(xb, 0, 0)
        put(0, six(xb, 0, wxv, 0))

        @pl.loop(0, steps)
        def _(t):
            par = lax.rem(t, 2)
            nxt = 1 - par

            @pl.when(t == 0)
            def _():
                load_xd.wait()
                load_xbc.wait()

            put(3, six(xb, t, wxv, 768))
            put(1, six(xb, t, wxv, 256))
            put(2, six(xb, t, wxv, 512))
            wait_rows(hb, par, h_slot + par)

            @pl.when(t == 0)
            def _():
                load_z.wait()

            add(1, six(hb, par, wzv, 256))
            add(2, six(hb, par, wzv, 512))
            wait_cols(xb, t, t)
            wait_cols(hb, par, h_slot + par)

            @pl.when(t < steps - 1)
            def _():
                load_frame(t + 1).wait()
                send(xb, t + 1, t + 1)

            b_vals = total(1, last(t, 256, hb, par, wzv, 256))
            for q in range(2):
                update_part(b_vals[q][..., :L], 2, q)
                reset_part(b_vals[q][..., L:], 0, q, par)
            c_vals = total(2, last(t, 512, hb, par, wzv, 512))
            for q in range(2):
                reset_part(c_vals[q][..., :L], 1, q, par)
                reset_part(c_vals[q][..., L:], 2, q, par)
            add(0, six(hb, par, wzv, 0))
            send(rb, par, r_slot + par)

            @pl.when(t == 0)
            def _():
                load_xe.wait()
                load_n.wait()

            a_vals = total(0, last(t, 0, hb, par, wzv, 0))
            for q in range(2):
                update_part(a_vals[q][..., :L], 0, q)
                update_part(a_vals[q][..., L:], 1, q)
            put(4, six(xb, t, wxv, 1024, L))
            wait_rows(rb, par, r_slot + par)
            add(3, six(rb, par, wnv, 0))
            add(4, six(rb, par, wnv, 256, L))
            wait_cols(rb, par, r_slot + par)

            @pl.when(t > 0)
            def _():
                store_step(t - 1, par).wait()

            d_vals = total(3, last(t, 768, rb, par, wnv, 0))
            for q in range(2):
                state_part(d_vals[q][..., :L], 0, q, nxt)
                state_part(d_vals[q][..., L:], 1, q, nxt)
            add(4, last(t, 1024, rb, par, wnv, 256, L))

            def finish():
                for q in range(2):
                    state_part(gv[(4,) + at(q) + lanes(0)], 2, q, nxt)

            @pl.when(t < steps - 1)
            def _():
                wait_rows(xb, t + 1, t + 1)
                finish()
                put(0, six(xb, t + 1, wxv, 0))
                send(hb, nxt, h_slot + nxt)
                store_step(t, nxt).start()

            @pl.when(t == steps - 1)
            def _():
                finish()
                store_step(t, nxt).start()

        store_last = pltpu.make_async_copy(hf, h_last, load_sem.at[steps])
        store_last.start()
        store_step(steps - 1, steps % 2).wait()
        store_last.wait()

    return kernel


def solution(mesh):
    n_cols = mesh.shape['cols']
    frame_spec = P(None, 'batch', 'rows', 'cols', None)
    state_spec = P('batch', 'rows', 'cols', None)

    def local_fn(frames, h_init, w_x, w_hzr, w_hn, gate_bias):
        steps, batch, tile_h, tile_w, ch = frames.shape
        pad = (tile_h + 2, tile_w + 2, batch, ch)
        tile = (tile_h, tile_w, batch, ch)
        vmem = pltpu.VMEM
        any_spec = pl.BlockSpec(memory_space=pl.ANY)
        h_seq, h_last = pl.pallas_call(
            make_kernel(steps, tile_h, tile_w, batch, ch, n_cols),
            out_shape=(jax.ShapeDtypeStruct((steps,) + tile, BF), jax.ShapeDtypeStruct(tile, F32)),
            in_specs=[any_spec] * 5 + [pl.BlockSpec(memory_space=pltpu.VMEM)],
            out_specs=(any_spec, any_spec),
            scratch_shapes=[
                vmem((steps,) + pad, BF), vmem((2,) + pad, BF), vmem((2,) + pad, BF),
                vmem(tile, F32), vmem(tile, F32),
                vmem((5,) + tile[:3] + (256,), F32),
                vmem((9 * ch, 3 * ch), BF), vmem((9 * ch, 2 * ch), BF), vmem((9 * ch, ch), BF),
                pltpu.SemaphoreType.DMA((steps + 4, 5)), pltpu.SemaphoreType.DMA((steps + 4, 5)),
                pltpu.SemaphoreType.DMA((steps + 7,)), pltpu.SemaphoreType.DMA((2,)),
            ],
            compiler_params=pltpu.CompilerParams(collective_id=0, has_side_effects=True, vmem_limit_bytes=60 * 1024 * 1024),
            name='convgru',
        )(
            jnp.transpose(frames, (0, 2, 3, 1, 4)),
            jnp.transpose(h_init, (1, 2, 0, 3)),
            w_x.reshape(9 * ch, -1), w_hzr.reshape(9 * ch, -1), w_hn.reshape(9 * ch, -1), gate_bias.reshape(1, -1),
        )
        return jnp.transpose(h_seq, (0, 3, 1, 2, 4)), jnp.transpose(h_last, (2, 0, 1, 3))

    return jax.shard_map(local_fn, mesh=mesh, in_specs=(frame_spec, state_spec, P(), P(), P(), P()),
                         out_specs=(frame_spec, state_spec), check_vma=False)
```

```python
import jax
import jax.numpy as jnp
from jax import lax
from jax.experimental import pallas as pl
from jax.experimental.pallas import tpu as pltpu
from jax.sharding import PartitionSpec as P

MESH = pl.DeviceIdType.MESH
BF = jnp.bfloat16
F32 = jnp.float32
L = 128


def sigmoid(v):
    return 0.5 * jnp.tanh(0.5 * v) + 0.5


def make_kernel(steps, tile_h, tile_w, batch, ch, n_cols):
    half_w = tile_w // 2

    def kernel(frames, h0, wx, wz, wn, bias, h_seq, h_last,
               xs, hs, pm, xb, hb, rb, hf, zf, gv, wxv, wzv, wnv, send_sem, recv_sem, load_sem, out_sem):
        row = lax.axis_index('rows')
        col = lax.axis_index('cols')
        has_left = col > 0
        has_right = col < n_cols - 1
        left, right, other = col - 1, col + 1, 1 - row
        src_row = tile_h - (tile_h - 1) * row
        dst_row = (tile_h + 1) * row

        inner = (pl.ds(1, tile_h), pl.ds(1, tile_w))

        def load_frame(t):
            return pltpu.make_async_copy(frames.at[t], xs.at[t], load_sem.at[t])

        def load_w(src, dst, first, width, sem):
            return pltpu.make_async_copy(src.at[:, pl.ds(first, width)], dst.at[:, pl.ds(first, width)], load_sem.at[sem])

        s0 = steps + 1
        load_h = [pltpu.make_async_copy(h0.at[:, pl.ds(g * L, L)], hs.at[g], load_sem.at[s0 + 6 + g]) for g in range(ch // L)]
        load_xa = load_w(wx, wxv, 0, 256, s0)
        load_xd = load_w(wx, wxv, 768, 256, s0 + 1)
        load_xbc = load_w(wx, wxv, 256, 512, s0 + 2)
        load_z = load_w(wz, wzv, 0, 768, s0 + 3)
        load_xe = load_w(wx, wxv, 1024, 128, s0 + 4)
        load_n = load_w(wn, wnv, 0, 384, s0 + 5)
        load_frame(0).start()
        load_xa.start()
        for cp in load_h:
            cp.start()
        load_xd.start()
        load_xbc.start()
        load_z.start()
        load_xe.start()
        load_n.start()
        for t in range(1, steps):
            load_frame(t).start()

        def zero_border(buf, i):
            edge = jnp.zeros((tile_w + 2, batch, ch), BF)
            buf[i, 0] = edge
            buf[i, tile_h + 1] = edge
            side = jnp.zeros((tile_h, 1, batch, ch), BF)
            buf[i, 1:tile_h + 1, 0:1] = side
            buf[i, 1:tile_h + 1, tile_w + 1:tile_w + 2] = side

        for i in range(2):
            zero_border(hb, i)
            zero_border(rb, i)

        @pl.loop(0, steps)
        def _(t):
            zero_border(xb, t)

        barrier = pltpu.get_barrier_semaphore()

        def greet(c, r):
            pl.semaphore_signal(barrier, inc=1, device_id={'cols': c, 'rows': r}, device_id_type=MESH)

        greet(col, other)

        @pl.when(has_left)
        def _():
            greet(left, row)
            greet(left, other)

        @pl.when(has_right)
        def _():
            greet(right, row)
            greet(right, other)

        pl.semaphore_wait(barrier, 1 + 2 * jnp.minimum(col, 1) + 2 * jnp.minimum(n_cols - 1 - col, 1))

        def copies(buf, i, slot):
            def rc(src, dst, k, c, r):
                return pltpu.make_async_remote_copy(
                    src_ref=buf.at[(i,) + src], dst_ref=buf.at[(i,) + dst], send_sem=send_sem.at[slot, k],
                    recv_sem=recv_sem.at[slot, k], device_id={'cols': c, 'rows': r}, device_id_type=MESH)
            rows = pl.ds(1, tile_h)
            return (
                rc((src_row, pl.ds(1, tile_w)), (dst_row, pl.ds(1, tile_w)), 0, col, other),
                rc((rows, 1), (rows, tile_w + 1), 1, left, row),
                rc((rows, tile_w), (rows, 0), 2, right, row),
                rc((src_row, 1), (dst_row, tile_w + 1), 3, left, other),
                rc((src_row, tile_w), (dst_row, 0), 4, right, other),
            )

        def send(buf, i, slot):
            cp = copies(buf, i, slot)
            cp[0].start()

            @pl.when(has_left)
            def _():
                cp[1].start()
                cp[3].start()

            @pl.when(has_right)
            def _():
                cp[2].start()
                cp[4].start()

        def wait_rows(buf, i, slot):
            copies(buf, i, slot)[0].wait_recv()

        def wait_cols(buf, i, slot):
            cp = copies(buf, i, slot)
            cp[0].wait_send()

            @pl.when(has_left)
            def _():
                cp[2].wait_recv()
                cp[4].wait_recv()
                cp[1].wait_send()
                cp[3].wait_send()

            @pl.when(has_right)
            def _():
                cp[1].wait_recv()
                cp[3].wait_recv()
                cp[2].wait_send()
                cp[4].wait_send()

        def dot(lhs, rhs, rows, cols):
            return jnp.dot(jnp.concatenate(lhs, axis=1), jnp.concatenate(rhs, axis=0),
                           preferred_element_type=F32).reshape(rows, cols, batch, -1)

        def view(buf, i, a, rows, c, c0, c1):
            return buf[i, a:a + rows, c0 + c:c1 + c].reshape(rows * (c1 - c0) * batch, ch)

        def part(srcs, cs, c0, c1, n):
            if n > L:
                lhs, rhs = [], []
                for (buf, i, w, first) in srcs:
                    for c in cs:
                        for a in range(3):
                            lhs.append(view(buf, i, a, tile_h, c, c0, c1))
                            rhs.append(w[(a * 3 + c) * ch:(a * 3 + c + 1) * ch, first:first + n])
                return dot(lhs, rhs, tile_h, c1 - c0)
            lhs, rhs, lhs_2, rhs_2 = [], [], [], []
            for (buf, i, w, first) in srcs:
                for c in cs:
                    tap = [w[(a * 3 + c) * ch:(a * 3 + c + 1) * ch, first:first + n] for a in range(3)]
                    lhs.append(view(buf, i, 0, tile_h + 1, c, c0, c1))
                    rhs.append(jnp.concatenate(tap[:2], axis=1))
                    lhs_2.append(view(buf, i, 2, tile_h, c, c0, c1))
                    rhs_2.append(tap[2])
            pair = dot(lhs, rhs, tile_h + 1, c1 - c0)
            return pair[:tile_h, :, :, :L] + pair[1:, :, :, L:] + dot(lhs_2, rhs_2, tile_h, c1 - c0)

        halves = (((1, 2), 0, half_w), ((1, 0), half_w, tile_w))
        inner_far = (((0,), 1, half_w), ((2,), half_w, tile_w - 1))
        edge_far = (((0,), 0, 1), ((2,), tile_w - 1, tile_w))

        def slot_at(s, c0, c1, n):
            return (s, slice(None), slice(c0, c1), slice(None), slice(0, n))

        def put(s, srcs, n=256, which=halves):
            for (cs, c0, c1) in which:
                gv[slot_at(s, c0, c1, n)] = part(srcs, cs, c0, c1, n)

        def add(s, srcs, n=256, which=halves):
            for (cs, c0, c1) in which:
                idx = slot_at(s, c0, c1, n)
                gv[idx] = gv[idx] + part(srcs, cs, c0, c1, n)

        def finish(s, srcs, which, end, n=256):
            for (cs, c0, c1) in which:
                end(gv[slot_at(s, c0, c1, n)] + part(srcs, cs, c0, c1, n), c0, c1)

        def lanes(g):
            return (slice(None), slice(g * L, (g + 1) * L))

        def at(c0, c1):
            return (slice(None), slice(c0, c1))

        def at_pad(c0, c1):
            return (slice(1, tile_h + 1), slice(1 + c0, 1 + c1))

        def b_of(first):
            return bias[first:first + L].reshape(1, 1, 1, L)

        def reset_part(v, g, c0, c1, par):
            r = sigmoid(v + b_of(ch + g * L))
            rb[(par,) + at_pad(c0, c1) + lanes(g)] = (r * hf[at(c0, c1) + lanes(g)]).astype(BF)

        def update_part(v, g, c0, c1):
            zf[at(c0, c1) + lanes(g)] = sigmoid(v + b_of(g * L))

        def state_part(v, g, c0, c1, nxt):
            idx = at(c0, c1) + lanes(g)
            n = jnp.tanh(v + b_of(2 * ch + g * L))
            z = zf[idx]
            h = (1.0 - z) * n + z * hf[idx]
            hf[idx] = h
            hb[(nxt,) + at_pad(c0, c1) + lanes(g)] = h.astype(BF)

        def end_a(v, c0, c1):
            update_part(v[..., :L], 0, c0, c1)
            update_part(v[..., L:], 1, c0, c1)

        def end_b(par):
            def end(v, c0, c1):
                update_part(v[..., :L], 2, c0, c1)
                reset_part(v[..., L:], 0, c0, c1, par)
            return end

        def end_c(par):
            def end(v, c0, c1):
                reset_part(v[..., :L], 1, c0, c1, par)
                reset_part(v[..., L:], 2, c0, c1, par)
            return end

        def end_d(nxt):
            def end(v, c0, c1):
                state_part(v[..., :L], 0, c0, c1, nxt)
                state_part(v[..., L:], 1, c0, c1, nxt)
            return end

        def end_e(nxt):
            def end(v, c0, c1):
                state_part(v, 2, c0, c1, nxt)
            return end

        def permute_frame(t):
            for j in range(tile_h // 2):
                rows = [xs[t, b * tile_h * tile_w + j * 2 * tile_w:b * tile_h * tile_w + (j + 1) * 2 * tile_w] for b in range(batch)]
                out = jnp.dot(pm[...], jnp.concatenate(rows, axis=0), preferred_element_type=F32)
                xb[t, 1 + 2 * j:3 + 2 * j, 1:tile_w + 1] = out.astype(BF).reshape(2, tile_w, batch, ch)

        def make_permutation():
            n = 2 * tile_w * batch
            o = lax.broadcasted_iota(jnp.int32, (n, n), 0)
            i = lax.broadcasted_iota(jnp.int32, (n, n), 1)
            src = (o & 15) * 16 + (o >> 7) * 8 + ((o >> 4) & 7)
            pm[...] = jnp.where(i == src, 1.0, 0.0).astype(BF)

        def permute_state():
            @pl.loop(0, tile_h)
            def _(r):
                for c in range(tile_w):
                    for g in range(ch // L):
                        v = hs[g, pl.ds(r * tile_w + c, batch, stride=tile_h * tile_w), :]
                        hf[r, c, :, g * L:(g + 1) * L] = v
                        hb[0, 1 + r, 1 + c, :, g * L:(g + 1) * L] = v.astype(BF)

        def store_step(t, nxt):
            return pltpu.make_async_copy(hb.at[(nxt,) + inner], h_seq.at[t], out_sem.at[nxt])

        h_slot, r_slot = steps, steps + 2

        make_permutation()
        load_frame(0).wait()
        permute_frame(0)
        send(xb, 0, 0)
        for cp in load_h:
            cp.wait()
        permute_state()
        send(hb, 0, h_slot)
        load_xa.wait()
        wait_rows(xb, 0, 0)
        put(0, [(xb, 0, wxv, 0)], which=halves[:1])

        @pl.loop(0, steps)
        def _(t):
            par = lax.rem(t, 2)
            nxt = 1 - par

            @pl.when(t == 0)
            def _():
                load_xd.wait()
                load_xbc.wait()

            put(0, [(xb, t, wxv, 0)], which=halves[1:])
            put(3, [(xb, t, wxv, 768)])
            put(1, [(xb, t, wxv, 256)])
            put(2, [(xb, t, wxv, 512)])

            @pl.when(t < steps - 1)
            def _():
                load_frame(t + 1).wait()
                permute_frame(t + 1)

            wait_rows(hb, par, h_slot + par)

            @pl.when(t == 0)
            def _():
                load_z.wait()

            add(1, [(hb, par, wzv, 256)])
            add(2, [(hb, par, wzv, 512)])
            both_b = [(xb, t, wxv, 256), (hb, par, wzv, 256)]
            both_c = [(xb, t, wxv, 512), (hb, par, wzv, 512)]
            finish(1, both_b, inner_far, end_b(par))
            finish(2, both_c, inner_far, end_c(par))
            wait_cols(xb, t, t)
            wait_cols(hb, par, h_slot + par)

            @pl.when(t < steps - 1)
            def _():
                send(xb, t + 1, t + 1)

            both_a = [(xb, t, wxv, 0), (hb, par, wzv, 0)]
            finish(1, both_b, edge_far, end_b(par))
            finish(2, both_c, edge_far, end_c(par))
            add(0, both_a, which=edge_far)
            send(rb, par, r_slot + par)

            @pl.when(t == 0)
            def _():
                load_xe.wait()
                load_n.wait()

            add(0, [(hb, par, wzv, 0)])
            finish(0, both_a, inner_far, end_a)
            for (_, c0, c1) in edge_far:
                end_a(gv[slot_at(0, c0, c1, 256)], c0, c1)
            put(4, [(xb, t, wxv, 1024)], n=L)
            wait_rows(rb, par, r_slot + par)

            @pl.when(t > 0)
            def _():
                store_step(t - 1, par).wait()

            both_d = [(xb, t, wxv, 768), (rb, par, wnv, 0)]
            both_e = [(xb, t, wxv, 1024), (rb, par, wnv, 256)]
            add(3, [(rb, par, wnv, 0)])
            add(4, [(rb, par, wnv, 256)], n=L)
            finish(3, both_d, inner_far, end_d(nxt))
            finish(4, both_e, inner_far, end_e(nxt), n=L)
            wait_cols(rb, par, r_slot + par)

            @pl.when(t < steps - 1)
            def _():
                wait_rows(xb, t + 1, t + 1)

            finish(3, both_d, edge_far, end_d(nxt))
            finish(4, both_e, edge_far, end_e(nxt), n=L)

            @pl.when(t < steps - 1)
            def _():
                put(0, [(xb, t + 1, wxv, 0)], which=halves[:1])
                send(hb, nxt, h_slot + nxt)

            store_step(t, nxt).start()

        store_last = pltpu.make_async_copy(hf, h_last, load_sem.at[steps])
        store_last.start()
        store_step(steps - 1, steps % 2).wait()
        store_last.wait()

    return kernel


def solution(mesh):
    n_cols = mesh.shape['cols']
    frame_spec = P(None, 'batch', 'rows', 'cols', None)
    state_spec = P('batch', 'rows', 'cols', None)

    def local_fn(frames, h_init, w_x, w_hzr, w_hn, gate_bias):
        steps, batch, tile_h, tile_w, ch = frames.shape
        pad = (tile_h + 2, tile_w + 2, batch, ch)
        tile = (tile_h, tile_w, batch, ch)
        vmem = pltpu.VMEM
        any_spec = pl.BlockSpec(memory_space=pl.ANY)
        h_seq, h_last = pl.pallas_call(
            make_kernel(steps, tile_h, tile_w, batch, ch, n_cols),
            out_shape=(jax.ShapeDtypeStruct((steps,) + tile, BF), jax.ShapeDtypeStruct(tile, F32)),
            in_specs=[any_spec] * 5 + [pl.BlockSpec(memory_space=pltpu.VMEM)],
            out_specs=(any_spec, any_spec),
            scratch_shapes=[
                vmem((steps, tile_h * tile_w * batch, ch), BF), vmem((ch // L, tile_h * tile_w * batch, L), F32),
                vmem((2 * tile_w * batch, 2 * tile_w * batch), BF),
                vmem((steps,) + pad, BF), vmem((2,) + pad, BF), vmem((2,) + pad, BF),
                vmem(tile, F32), vmem(tile, F32),
                vmem((5,) + tile[:3] + (256,), F32),
                vmem((9 * ch, 3 * ch), BF), vmem((9 * ch, 2 * ch), BF), vmem((9 * ch, ch), BF),
                pltpu.SemaphoreType.DMA((steps + 4, 5)), pltpu.SemaphoreType.DMA((steps + 4, 5)),
                pltpu.SemaphoreType.DMA((steps + 10,)), pltpu.SemaphoreType.DMA((2,)),
            ],
            compiler_params=pltpu.CompilerParams(collective_id=0, has_side_effects=True, vmem_limit_bytes=60 * 1024 * 1024),
            name='convgru',
        )(
            frames.reshape(steps, -1, ch), h_init.reshape(-1, ch),
            w_x.reshape(9 * ch, -1), w_hzr.reshape(9 * ch, -1), w_hn.reshape(9 * ch, -1), gate_bias,
        )
        return jnp.transpose(h_seq, (0, 3, 1, 2, 4)), jnp.transpose(h_last, (2, 0, 1, 3))

    return jax.shard_map(local_fn, mesh=mesh, in_specs=(frame_spec, state_spec, P(), P(), P(), P()),
                         out_specs=(frame_spec, state_spec), check_vma=False)
```

```python
import jax
import jax.numpy as jnp
from jax import lax
from jax.experimental import pallas as pl
from jax.experimental.pallas import tpu as pltpu
from jax.sharding import PartitionSpec as P

MESH = pl.DeviceIdType.MESH
BF = jnp.bfloat16
F32 = jnp.float32
L = 128


def sigmoid(v):
    return 0.5 * jnp.tanh(0.5 * v) + 0.5


def make_kernel(steps, tile_h, tile_w, batch, ch, n_cols):
    half_w = tile_w // 2

    def kernel(frames, h0, wx, wz, wn, bias, h_seq, h_last,
               xs, hs, pm, xb, hb, rb, hf, zf, gv, wxv, wzv, wnv, send_sem, recv_sem, load_sem, out_sem):
        row = lax.axis_index('rows')
        col = lax.axis_index('cols')
        left, right, other = (col + n_cols - 1) % n_cols, (col + 1) % n_cols, 1 - row
        spare = tile_w + 2
        to_left = tile_w + 1 + (n_cols - col) // n_cols
        to_right = spare * ((col + 1) // n_cols)
        src_row = tile_h - (tile_h - 1) * row
        dst_row = (tile_h + 1) * row

        inner = (pl.ds(1, tile_h), pl.ds(1, tile_w))

        def load_frame(t):
            return pltpu.make_async_copy(frames.at[t], xs.at[t], load_sem.at[t])

        def load_w(src, dst, first, width, sem):
            return pltpu.make_async_copy(src.at[:, pl.ds(first, width)], dst.at[:, pl.ds(first, width)], load_sem.at[sem])

        s0 = steps + 1
        load_h = [pltpu.make_async_copy(h0.at[:, pl.ds(g * L, L)], hs.at[g], load_sem.at[s0 + 6 + g]) for g in range(ch // L)]
        load_xabc = load_w(wx, wxv, 0, 768, s0)
        load_xd = load_w(wx, wxv, 768, 256, s0 + 1)
        load_z = load_w(wz, wzv, 0, 768, s0 + 3)
        load_xe = load_w(wx, wxv, 1024, 128, s0 + 4)
        load_n = load_w(wn, wnv, 0, 384, s0 + 5)
        load_frame(0).start()
        for cp in load_h:
            cp.start()
        load_xabc.start()
        for t in range(1, steps):
            load_frame(t).start()
        load_z.start()
        load_xd.start()
        load_xe.start()
        load_n.start()

        def zero_border(buf, i):
            edge = jnp.zeros((tile_w + 3, batch, ch), BF)
            buf[i, 0] = edge
            buf[i, tile_h + 1] = edge
            side = jnp.zeros((tile_h, 1, batch, ch), BF)
            buf[i, 1:tile_h + 1, 0:1] = side
            buf[i, 1:tile_h + 1, tile_w + 1:tile_w + 2] = side

        for i in range(2):
            zero_border(hb, i)
            zero_border(rb, i)

        @pl.loop(0, steps)
        def _(t):
            zero_border(xb, t)

        barrier = pltpu.get_barrier_semaphore()

        def greet(c, r):
            pl.semaphore_signal(barrier, inc=1, device_id={'cols': c, 'rows': r}, device_id_type=MESH)

        greet(col, other)
        for side_col in (left, right):
            greet(side_col, row)
            greet(side_col, other)
        pl.semaphore_wait(barrier, 5)

        def copies(buf, i, slot):
            def rc(src, dst, k, c, r):
                return pltpu.make_async_remote_copy(
                    src_ref=buf.at[(i,) + src], dst_ref=buf.at[(i,) + dst], send_sem=send_sem.at[slot, k],
                    recv_sem=recv_sem.at[slot, k], device_id={'cols': c, 'rows': r}, device_id_type=MESH)
            rows = pl.ds(1, tile_h)
            return (
                rc((src_row, pl.ds(1, tile_w)), (dst_row, pl.ds(1, tile_w)), 0, col, other),
                rc((rows, 1), (rows, to_left), 1, left, row),
                rc((rows, tile_w), (rows, to_right), 2, right, row),
                rc((src_row, 1), (dst_row, to_left), 3, left, other),
                rc((src_row, tile_w), (dst_row, to_right), 4, right, other),
            )

        def send(buf, i, slot):
            for cp in copies(buf, i, slot):
                cp.start()

        def wait_rows(buf, i, slot):
            copies(buf, i, slot)[0].wait_recv()

        def wait_cols(buf, i, slot):
            cps = copies(buf, i, slot)
            for cp in cps[1:]:
                cp.wait_recv()
            for cp in cps:
                cp.wait_send()

        def dot(lhs, rhs, rows, cols):
            return jnp.dot(jnp.concatenate(lhs, axis=1), jnp.concatenate(rhs, axis=0),
                           preferred_element_type=F32).reshape(rows, cols, batch, -1)

        def view(buf, i, a, rows, c, c0, c1):
            return buf[i, a:a + rows, c0 + c:c1 + c].reshape(rows * (c1 - c0) * batch, ch)

        def part(srcs, cs, c0, c1, n):
            if n > L:
                lhs, rhs = [], []
                for (buf, i, w, first) in srcs:
                    for c in cs:
                        for a in range(3):
                            lhs.append(view(buf, i, a, tile_h, c, c0, c1))
                            rhs.append(w[(a * 3 + c) * ch:(a * 3 + c + 1) * ch, first:first + n])
                return dot(lhs, rhs, tile_h, c1 - c0)
            lhs, rhs, lhs_2, rhs_2 = [], [], [], []
            for (buf, i, w, first) in srcs:
                for c in cs:
                    tap = [w[(a * 3 + c) * ch:(a * 3 + c + 1) * ch, first:first + n] for a in range(3)]
                    lhs.append(view(buf, i, 0, tile_h + 1, c, c0, c1))
                    rhs.append(jnp.concatenate(tap[:2], axis=1))
                    lhs_2.append(view(buf, i, 2, tile_h, c, c0, c1))
                    rhs_2.append(tap[2])
            pair = dot(lhs, rhs, tile_h + 1, c1 - c0)
            return pair[:tile_h, :, :, :L] + pair[1:, :, :, L:] + dot(lhs_2, rhs_2, tile_h, c1 - c0)

        halves = (((1, 2), 0, half_w), ((1, 0), half_w, tile_w))
        inner_far = (((0,), 1, half_w), ((2,), half_w, tile_w - 1))
        edge_far = (((0,), 0, 1), ((2,), tile_w - 1, tile_w))

        def slot_at(s, c0, c1, n):
            return (s, slice(None), slice(c0, c1), slice(None), slice(0, n))

        def put(s, srcs, n=256, which=halves):
            for (cs, c0, c1) in which:
                gv[slot_at(s, c0, c1, n)] = part(srcs, cs, c0, c1, n)

        def add(s, srcs, n=256, which=halves):
            for (cs, c0, c1) in which:
                idx = slot_at(s, c0, c1, n)
                gv[idx] = gv[idx] + part(srcs, cs, c0, c1, n)

        def finish(s, srcs, which, end, n=256):
            for (cs, c0, c1) in which:
                end(gv[slot_at(s, c0, c1, n)] + part(srcs, cs, c0, c1, n), c0, c1)

        def lanes(g):
            return (slice(None), slice(g * L, (g + 1) * L))

        def at(c0, c1):
            return (slice(None), slice(c0, c1))

        def at_pad(c0, c1):
            return (slice(1, tile_h + 1), slice(1 + c0, 1 + c1))

        def b_of(first):
            return bias[first:first + L].reshape(1, 1, 1, L)

        def reset_part(v, g, c0, c1, par):
            r = sigmoid(v + b_of(ch + g * L))
            rb[(par,) + at_pad(c0, c1) + lanes(g)] = (r * hf[at(c0, c1) + lanes(g)]).astype(BF)

        def update_part(v, g, c0, c1):
            zf[at(c0, c1) + lanes(g)] = sigmoid(v + b_of(g * L))

        def state_part(v, g, c0, c1, nxt):
            idx = at(c0, c1) + lanes(g)
            n = jnp.tanh(v + b_of(2 * ch + g * L))
            z = zf[idx]
            h = (1.0 - z) * n + z * hf[idx]
            hf[idx] = h
            hb[(nxt,) + at_pad(c0, c1) + lanes(g)] = h.astype(BF)

        def end_a(v, c0, c1):
            update_part(v[..., :L], 0, c0, c1)
            update_part(v[..., L:], 1, c0, c1)

        def end_b(par):
            def end(v, c0, c1):
                update_part(v[..., :L], 2, c0, c1)
                reset_part(v[..., L:], 0, c0, c1, par)
            return end

        def end_c(par):
            def end(v, c0, c1):
                reset_part(v[..., :L], 1, c0, c1, par)
                reset_part(v[..., L:], 2, c0, c1, par)
            return end

        def end_d(nxt):
            def end(v, c0, c1):
                state_part(v[..., :L], 0, c0, c1, nxt)
                state_part(v[..., L:], 1, c0, c1, nxt)
            return end

        def end_e(nxt):
            def end(v, c0, c1):
                state_part(v, 2, c0, c1, nxt)
            return end

        def permute_frame(t):
            for j in range(tile_h // 2):
                rows = [xs[t, b * tile_h * tile_w + j * 2 * tile_w:b * tile_h * tile_w + (j + 1) * 2 * tile_w] for b in range(batch)]
                out = jnp.dot(pm[...], jnp.concatenate(rows, axis=0), preferred_element_type=F32)
                xb[t, 1 + 2 * j:3 + 2 * j, 1:tile_w + 1] = out.astype(BF).reshape(2, tile_w, batch, ch)

        def make_permutation():
            n = 2 * tile_w * batch
            o = lax.broadcasted_iota(jnp.int32, (n, n), 0)
            i = lax.broadcasted_iota(jnp.int32, (n, n), 1)
            src = (o & 15) * 16 + (o >> 7) * 8 + ((o >> 4) & 7)
            pm[...] = jnp.where(i == src, 1.0, 0.0).astype(BF)

        def permute_state():
            @pl.loop(0, tile_h)
            def _(r):
                for c in range(tile_w):
                    for g in range(ch // L):
                        v = hs[g, pl.ds(r * tile_w + c, batch, stride=tile_h * tile_w), :]
                        hf[r, c, :, g * L:(g + 1) * L] = v
                        hb[0, 1 + r, 1 + c, :, g * L:(g + 1) * L] = v.astype(BF)

        def store_step(t, nxt):
            return pltpu.make_async_copy(hb.at[(nxt,) + inner], h_seq.at[t], out_sem.at[nxt])

        h_slot, r_slot = steps, steps + 2

        make_permutation()
        load_frame(0).wait()
        permute_frame(0)
        send(xb, 0, 0)
        for cp in load_h:
            cp.wait()
        permute_state()
        send(hb, 0, h_slot)
        store_step(0, 0).start()
        for t in range(1, steps):
            load_frame(t).wait()
        for t in range(1, steps):
            permute_frame(t)
        load_xabc.wait()
        wait_rows(xb, 0, 0)

        @pl.loop(0, steps)
        def _(t):
            par = lax.rem(t, 2)
            nxt = 1 - par

            put(1, [(xb, t, wxv, 256)])
            put(2, [(xb, t, wxv, 512)])
            wait_rows(hb, par, h_slot + par)

            @pl.when(t == 0)
            def _():
                load_z.wait()

            add(1, [(hb, par, wzv, 256)])
            add(2, [(hb, par, wzv, 512)])
            both_b = [(xb, t, wxv, 256), (hb, par, wzv, 256)]
            both_c = [(xb, t, wxv, 512), (hb, par, wzv, 512)]
            finish(1, both_b, inner_far, end_b(par))
            finish(2, both_c, inner_far, end_c(par))
            put(0, [(xb, t, wxv, 0)])
            wait_cols(xb, t, t)
            wait_cols(hb, par, h_slot + par)
            store_step(jnp.maximum(t - 1, 0), par).wait()
            both_a = [(xb, t, wxv, 0), (hb, par, wzv, 0)]
            finish(1, both_b, edge_far, end_b(par))
            finish(2, both_c, edge_far, end_c(par))
            add(0, both_a, which=edge_far)
            send(rb, par, r_slot + par)

            @pl.when(t < steps - 1)
            def _():
                send(xb, t + 1, t + 1)

            @pl.when(t == 0)
            def _():
                load_xd.wait()
                load_xe.wait()
                load_n.wait()

            add(0, [(hb, par, wzv, 0)])
            finish(0, both_a, inner_far, end_a)
            for (_, c0, c1) in edge_far:
                end_a(gv[slot_at(0, c0, c1, 256)], c0, c1)
            put(3, [(xb, t, wxv, 768)])
            wait_rows(rb, par, r_slot + par)


            put(4, [(xb, t, wxv, 1024)], n=L)
            both_d = [(xb, t, wxv, 768), (rb, par, wnv, 0)]
            both_e = [(xb, t, wxv, 1024), (rb, par, wnv, 256)]
            add(3, [(rb, par, wnv, 0)])
            add(4, [(rb, par, wnv, 256)], n=L)
            finish(3, both_d, inner_far, end_d(nxt))
            finish(4, both_e, inner_far, end_e(nxt), n=L)
            wait_cols(rb, par, r_slot + par)
            finish(3, both_d, edge_far, end_d(nxt))
            finish(4, both_e, edge_far, end_e(nxt), n=L)

            @pl.when(t < steps - 1)
            def _():
                send(hb, nxt, h_slot + nxt)
                wait_rows(xb, t + 1, t + 1)

            store_step(t, nxt).start()

        store_last = pltpu.make_async_copy(hf, h_last, load_sem.at[steps])
        store_last.start()
        store_step(steps - 1, steps % 2).wait()
        store_last.wait()

    return kernel


def solution(mesh):
    n_cols = mesh.shape['cols']
    frame_spec = P(None, 'batch', 'rows', 'cols', None)
    state_spec = P('batch', 'rows', 'cols', None)

    def local_fn(frames, h_init, w_x, w_hzr, w_hn, gate_bias):
        steps, batch, tile_h, tile_w, ch = frames.shape
        pad = (tile_h + 2, tile_w + 3, batch, ch)
        tile = (tile_h, tile_w, batch, ch)
        vmem = pltpu.VMEM
        any_spec = pl.BlockSpec(memory_space=pl.ANY)
        h_seq, h_last = pl.pallas_call(
            make_kernel(steps, tile_h, tile_w, batch, ch, n_cols),
            out_shape=(jax.ShapeDtypeStruct((steps,) + tile, BF), jax.ShapeDtypeStruct(tile, F32)),
            in_specs=[any_spec] * 5 + [pl.BlockSpec(memory_space=pltpu.VMEM)],
            out_specs=(any_spec, any_spec),
            scratch_shapes=[
                vmem((steps, tile_h * tile_w * batch, ch), BF), vmem((ch // L, tile_h * tile_w * batch, L), F32),
                vmem((2 * tile_w * batch, 2 * tile_w * batch), BF),
                vmem((steps,) + pad, BF), vmem((2,) + pad, BF), vmem((2,) + pad, BF),
                vmem(tile, F32), vmem(tile, F32),
                vmem((5,) + tile[:3] + (256,), F32),
                vmem((9 * ch, 3 * ch), BF), vmem((9 * ch, 2 * ch), BF), vmem((9 * ch, ch), BF),
                pltpu.SemaphoreType.DMA((steps + 4, 5)), pltpu.SemaphoreType.DMA((steps + 4, 5)),
                pltpu.SemaphoreType.DMA((steps + 10,)), pltpu.SemaphoreType.DMA((2,)),
            ],
            compiler_params=pltpu.CompilerParams(collective_id=0, has_side_effects=True, vmem_limit_bytes=60 * 1024 * 1024),
            name='convgru',
        )(
            frames.reshape(steps, -1, ch), h_init.reshape(-1, ch),
            w_x.reshape(9 * ch, -1), w_hzr.reshape(9 * ch, -1), w_hn.reshape(9 * ch, -1), gate_bias,
        )
        return jnp.transpose(h_seq, (0, 3, 1, 2, 4)), jnp.transpose(h_last, (2, 0, 1, 3))

    return jax.shard_map(local_fn, mesh=mesh, in_specs=(frame_spec, state_spec, P(), P(), P(), P()),
                         out_specs=(frame_spec, state_spec), check_vma=False)
```

```python
import jax
import jax.numpy as jnp
from jax import lax
from jax.experimental import pallas as pl
from jax.experimental.pallas import tpu as pltpu
from jax.sharding import PartitionSpec as P

MESH = pl.DeviceIdType.MESH
BF = jnp.bfloat16
F32 = jnp.float32
L = 128


def sigmoid(v):
    return 0.5 * jnp.tanh(0.5 * v) + 0.5


def make_kernel(steps, tile_h, tile_w, batch, ch, n_cols):
    half_w = tile_w // 2

    def kernel(frames, h0, wx, wz, wn, bias, h_seq, h_last,
               xs, hs, pm, xb, hb, rb, hf, zf, gv, wxv, wzv, wnv, send_sem, recv_sem, load_sem, out_sem):
        row = lax.axis_index('rows')
        col = lax.axis_index('cols')
        other = 1 - row
        first = (n_cols - col) // n_cols
        final = (col + 1) // n_cols
        left, right = col - 1 + first, col + 1 - final
        left_row, right_row = row + first * (1 - 2 * row), row + final * (1 - 2 * row)
        to_left, to_right = tile_w + 1 + first, final * (tile_w + 2)
        src_row = tile_h - (tile_h - 1) * row
        dst_row = (tile_h + 1) * row

        inner = (pl.ds(1, tile_h), pl.ds(1, tile_w))

        def load_frame(t):
            return pltpu.make_async_copy(frames.at[t], xs.at[t], load_sem.at[t])

        def load_w(src, dst, first, width, sem):
            return pltpu.make_async_copy(src.at[:, pl.ds(first, width)], dst.at[:, pl.ds(first, width)], load_sem.at[sem])

        s0 = steps + 1
        load_h = [pltpu.make_async_copy(h0.at[:, :, pl.ds(g * L, L)], hs.at[g, :, pl.ds(0, tile_h * tile_w)], load_sem.at[s0 + 6 + g])
                  for g in range(ch // L)]
        load_xbc = load_w(wx, wxv, 256, 512, s0)
        load_xa = load_w(wx, wxv, 0, 256, s0 + 2)
        load_xd = load_w(wx, wxv, 768, 256, s0 + 1)
        load_z = load_w(wz, wzv, 0, 768, s0 + 3)
        load_xe = load_w(wx, wxv, 1024, 128, s0 + 4)
        load_n = load_w(wn, wnv, 0, 384, s0 + 5)
        load_frame(0).start()
        for cp in load_h:
            cp.start()
        load_xbc.start()
        for t in range(1, steps):
            load_frame(t).start()
        load_xa.start()
        load_z.start()
        load_xd.start()
        load_xe.start()
        load_n.start()

        def zero_border(buf, i):
            edge = jnp.zeros((tile_w + 3, batch, ch), BF)
            buf[i, 0] = edge
            buf[i, tile_h + 1] = edge
            side = jnp.zeros((tile_h, 1, batch, ch), BF)
            buf[i, 1:tile_h + 1, 0:1] = side
            buf[i, 1:tile_h + 1, tile_w + 1:tile_w + 2] = side

        for i in range(2):
            zero_border(hb, i)
            zero_border(rb, i)

        @pl.loop(0, steps)
        def _(t):
            zero_border(xb, t)

        barrier = pltpu.get_barrier_semaphore()

        def greet(c, r):
            pl.semaphore_signal(barrier, inc=1, device_id={'cols': c, 'rows': r}, device_id_type=MESH)

        greet(col, other)
        greet(left, left_row)
        greet(left, other)
        greet(right, right_row)
        greet(right, other)
        pl.semaphore_wait(barrier, 5)

        def copies(buf, i, slot, first=first, final=final):
            def rc(src, dst, k, land, c, r):
                return pltpu.make_async_remote_copy(
                    src_ref=buf.at[(i,) + src], dst_ref=buf.at[(i,) + dst], send_sem=send_sem.at[slot, k],
                    recv_sem=recv_sem.at[slot, land], device_id={'cols': c, 'rows': r}, device_id_type=MESH)
            rows = pl.ds(1, tile_h)
            return (
                rc((src_row, pl.ds(1, tile_w)), (dst_row, pl.ds(1, tile_w)), 0, 0, col, other),
                rc((rows, 1), (rows, to_left), 1, 1 + first, left, left_row),
                rc((rows, tile_w), (rows, to_right), 2, 2 - final, right, right_row),
                rc((src_row, 1), (dst_row, to_left), 3, 3 + first, left, other),
                rc((src_row, tile_w), (dst_row, to_right), 4, 4 - final, right, other),
            )

        def send(buf, i, slot):
            for cp in copies(buf, i, slot):
                cp.start()

        def wait_rows(buf, i, slot):
            copies(buf, i, slot)[0].wait_recv()

        def wait_cols(buf, i, slot):
            for cp in copies(buf, i, slot, 0, 0)[1:]:
                cp.wait_recv()
            for cp in copies(buf, i, slot):
                cp.wait_send()

        def dot(lhs, rhs, rows, cols):
            return jnp.dot(jnp.concatenate(lhs, axis=1), jnp.concatenate(rhs, axis=0),
                           preferred_element_type=F32).reshape(rows, cols, batch, -1)

        def view(buf, i, a, rows, c, c0, c1):
            return buf[i, a:a + rows, c0 + c:c1 + c].reshape(rows * (c1 - c0) * batch, ch)

        def part(srcs, cs, c0, c1, n):
            if n > L:
                lhs, rhs = [], []
                for (buf, i, w, first) in srcs:
                    for c in cs:
                        for a in range(3):
                            lhs.append(view(buf, i, a, tile_h, c, c0, c1))
                            rhs.append(w[(a * 3 + c) * ch:(a * 3 + c + 1) * ch, first:first + n])
                return dot(lhs, rhs, tile_h, c1 - c0)
            lhs, rhs, lhs_2, rhs_2 = [], [], [], []
            both = len(cs) == 2
            low = min(cs)
            for (buf, i, w, first_n) in srcs:
                tap = {(a, c): w[(a * 3 + c) * ch:(a * 3 + c + 1) * ch, first_n:first_n + n] for c in cs for a in range(3)}
                for c in cs:
                    lhs.append(view(buf, i, 0, tile_h + 1, c, c0, c1))
                    rhs.append(jnp.concatenate([tap[0, c], tap[1, c]], axis=1))
                lhs_2.append(view(buf, i, 2, tile_h, low, c0, c1 + both))
                rhs_2.append(jnp.concatenate([tap[2, low], tap[2, low + 1]], axis=1) if both else tap[2, low])
            pair = dot(lhs, rhs, tile_h + 1, c1 - c0)
            out = pair[:tile_h, :, :, :L] + pair[1:, :, :, L:]
            pair = dot(lhs_2, rhs_2, tile_h, c1 - c0 + both)
            return out + (pair[:, :-1, :, :L] + pair[:, 1:, :, L:] if both else pair)

        halves = (((1, 2), 0, half_w), ((1, 0), half_w, tile_w))
        inner_far = (((0,), 1, half_w), ((2,), half_w, tile_w - 1))
        edge_far = (((0,), 0, 1), ((2,), tile_w - 1, tile_w))

        def slot_at(s, c0, c1, n):
            return (s, slice(None), slice(c0, c1), slice(None), slice(0, n))

        def put(s, srcs, n=256, which=halves):
            for (cs, c0, c1) in which:
                gv[slot_at(s, c0, c1, n)] = part(srcs, cs, c0, c1, n)

        def add(s, srcs, n=256, which=halves):
            for (cs, c0, c1) in which:
                idx = slot_at(s, c0, c1, n)
                gv[idx] = gv[idx] + part(srcs, cs, c0, c1, n)

        def finish(s, srcs, which, end, n=256):
            for (cs, c0, c1) in which:
                end(gv[slot_at(s, c0, c1, n)] + part(srcs, cs, c0, c1, n), c0, c1)

        def lanes(g):
            return (slice(None), slice(g * L, (g + 1) * L))

        def at(c0, c1):
            return (slice(None), slice(c0, c1))

        def at_pad(c0, c1):
            return (slice(1, tile_h + 1), slice(1 + c0, 1 + c1))

        def b_of(first):
            return bias[first:first + L].reshape(1, 1, 1, L)

        def reset_part(v, g, c0, c1, par):
            r = sigmoid(v + b_of(ch + g * L))
            rb[(par,) + at_pad(c0, c1) + lanes(g)] = (r * hf[at(c0, c1) + lanes(g)]).astype(BF)

        def update_part(v, g, c0, c1):
            zf[at(c0, c1) + lanes(g)] = sigmoid(v + b_of(g * L))

        def state_part(v, g, c0, c1, nxt):
            idx = at(c0, c1) + lanes(g)
            n = jnp.tanh(v + b_of(2 * ch + g * L))
            z = zf[idx]
            h = (1.0 - z) * n + z * hf[idx]
            hf[idx] = h
            hb[(nxt,) + at_pad(c0, c1) + lanes(g)] = h.astype(BF)

        def end_a(v, c0, c1):
            update_part(v[..., :L], 0, c0, c1)
            update_part(v[..., L:], 1, c0, c1)

        def end_b(par):
            def end(v, c0, c1):
                update_part(v[..., :L], 2, c0, c1)
                reset_part(v[..., L:], 0, c0, c1, par)
            return end

        def end_c(par):
            def end(v, c0, c1):
                reset_part(v[..., :L], 1, c0, c1, par)
                reset_part(v[..., L:], 2, c0, c1, par)
            return end

        def end_d(nxt):
            def end(v, c0, c1):
                state_part(v[..., :L], 0, c0, c1, nxt)
                state_part(v[..., L:], 1, c0, c1, nxt)
            return end

        def end_e(nxt):
            def end(v, c0, c1):
                state_part(v, 2, c0, c1, nxt)
            return end

        def permute_frame(t):
            for j in range(tile_h // 2):
                rows = [xs[t, b * tile_h * tile_w + j * 2 * tile_w:b * tile_h * tile_w + (j + 1) * 2 * tile_w] for b in range(batch)]
                out = jnp.dot(pm[...], jnp.concatenate(rows, axis=0), preferred_element_type=F32)
                xb[t, 1 + 2 * j:3 + 2 * j, 1:tile_w + 1] = out.astype(BF).reshape(2, tile_w, batch, ch)

        def make_permutation():
            n = 2 * tile_w * batch
            o = lax.broadcasted_iota(jnp.int32, (n, n), 0)
            i = lax.broadcasted_iota(jnp.int32, (n, n), 1)
            src = (o & 15) * 16 + (o >> 7) * 8 + ((o >> 4) & 7)
            pm[...] = jnp.where(i == src, 1.0, 0.0).astype(BF)

        pitch = tile_h * tile_w + 8

        def permute_state():
            @pl.loop(0, tile_h)
            def _(r):
                for c in range(tile_w):
                    for g in range(ch // L):
                        v = hs.at[g].reshape(batch * pitch, L)[pl.ds(r * tile_w + c, batch, stride=pitch), :]
                        hf[r, c, :, g * L:(g + 1) * L] = v
                        hb[0, 1 + r, 1 + c, :, g * L:(g + 1) * L] = v.astype(BF)

        def store_step(t, nxt):
            return pltpu.make_async_copy(hb.at[(nxt,) + inner], h_seq.at[t], out_sem.at[nxt])

        h_slot, r_slot = steps, steps + 2

        make_permutation()
        load_frame(0).wait()
        permute_frame(0)
        send(xb, 0, 0)
        for cp in load_h:
            cp.wait()
        permute_state()
        send(hb, 0, h_slot)
        store_step(0, 0).start()
        for t in range(1, steps):
            load_frame(t).wait()
        for t in range(1, steps):
            permute_frame(t)
        load_xbc.wait()
        wait_rows(xb, 0, 0)

        @pl.loop(0, steps)
        def _(t):
            par = lax.rem(t, 2)
            nxt = 1 - par

            put(1, [(xb, t, wxv, 256)])
            put(2, [(xb, t, wxv, 512)])
            wait_rows(hb, par, h_slot + par)

            @pl.when(t == 0)
            def _():
                load_xa.wait()
                load_z.wait()

            add(1, [(hb, par, wzv, 256)])
            add(2, [(hb, par, wzv, 512)])
            both_b = [(xb, t, wxv, 256), (hb, par, wzv, 256)]
            both_c = [(xb, t, wxv, 512), (hb, par, wzv, 512)]
            finish(1, both_b, inner_far, end_b(par))
            finish(2, both_c, inner_far, end_c(par))
            put(0, [(xb, t, wxv, 0)])
            wait_cols(xb, t, t)
            wait_cols(hb, par, h_slot + par)
            store_step(jnp.maximum(t - 1, 0), par).wait()
            both_a = [(xb, t, wxv, 0), (hb, par, wzv, 0)]
            finish(1, both_b, edge_far, end_b(par))
            finish(2, both_c, edge_far, end_c(par))
            add(0, both_a, which=edge_far)
            send(rb, par, r_slot + par)

            @pl.when(t < steps - 1)
            def _():
                send(xb, t + 1, t + 1)

            @pl.when(t == 0)
            def _():
                load_xd.wait()
                load_xe.wait()
                load_n.wait()

            add(0, [(hb, par, wzv, 0)])
            finish(0, both_a, inner_far, end_a)
            for (_, c0, c1) in edge_far:
                end_a(gv[slot_at(0, c0, c1, 256)], c0, c1)
            put(3, [(xb, t, wxv, 768)])
            wait_rows(rb, par, r_slot + par)


            both_d = [(xb, t, wxv, 768), (rb, par, wnv, 0)]
            both_e = [(xb, t, wxv, 1024), (rb, par, wnv, 256)]
            add(3, [(rb, par, wnv, 0)])
            put(4, both_e, n=L)
            finish(3, both_d, inner_far, end_d(nxt))
            finish(4, both_e, inner_far, end_e(nxt), n=L)
            wait_cols(rb, par, r_slot + par)
            finish(3, both_d, edge_far, end_d(nxt))
            finish(4, both_e, edge_far, end_e(nxt), n=L)

            @pl.when(t < steps - 1)
            def _():
                send(hb, nxt, h_slot + nxt)
                wait_rows(xb, t + 1, t + 1)

            store_step(t, nxt).start()

        store_last = pltpu.make_async_copy(hf, h_last, load_sem.at[steps])
        store_last.start()
        store_step(steps - 1, steps % 2).wait()
        store_last.wait()

    return kernel


def solution(mesh):
    n_cols = mesh.shape['cols']
    frame_spec = P(None, 'batch', 'rows', 'cols', None)
    state_spec = P('batch', 'rows', 'cols', None)

    def local_fn(frames, h_init, w_x, w_hzr, w_hn, gate_bias):
        steps, batch, tile_h, tile_w, ch = frames.shape
        pad = (tile_h + 2, tile_w + 3, batch, ch)
        tile = (tile_h, tile_w, batch, ch)
        vmem = pltpu.VMEM
        any_spec = pl.BlockSpec(memory_space=pl.ANY)
        h_seq, h_last = pl.pallas_call(
            make_kernel(steps, tile_h, tile_w, batch, ch, n_cols),
            out_shape=(jax.ShapeDtypeStruct((steps,) + tile, BF), jax.ShapeDtypeStruct(tile, F32)),
            in_specs=[any_spec] * 5 + [pl.BlockSpec(memory_space=pltpu.VMEM)],
            out_specs=(any_spec, any_spec),
            scratch_shapes=[
                vmem((steps, tile_h * tile_w * batch, ch), BF), vmem((ch // L, batch, tile_h * tile_w + 8, L), F32),
                vmem((2 * tile_w * batch, 2 * tile_w * batch), BF),
                vmem((steps,) + pad, BF), vmem((2,) + pad, BF), vmem((2,) + pad, BF),
                vmem(tile, F32), vmem(tile, F32),
                vmem((5,) + tile[:3] + (256,), F32),
                vmem((9 * ch, 3 * ch), BF), vmem((9 * ch, 2 * ch), BF), vmem((9 * ch, ch), BF),
                pltpu.SemaphoreType.DMA((steps + 4, 5)), pltpu.SemaphoreType.DMA((steps + 4, 5)),
                pltpu.SemaphoreType.DMA((steps + 10,)), pltpu.SemaphoreType.DMA((2,)),
            ],
            compiler_params=pltpu.CompilerParams(collective_id=0, has_side_effects=True, vmem_limit_bytes=60 * 1024 * 1024),
            name='convgru',
        )(
            frames.reshape(steps, -1, ch), h_init.reshape(batch, -1, ch),
            w_x.reshape(9 * ch, -1), w_hzr.reshape(9 * ch, -1), w_hn.reshape(9 * ch, -1), gate_bias,
        )
        return jnp.transpose(h_seq, (0, 3, 1, 2, 4)), jnp.transpose(h_last, (2, 0, 1, 3))

    return jax.shard_map(local_fn, mesh=mesh, in_specs=(frame_spec, state_spec, P(), P(), P(), P()),
                         out_specs=(frame_spec, state_spec), check_vma=False)
```

```python
import jax
import jax.numpy as jnp
from jax import lax
from jax.experimental import pallas as pl
from jax.experimental.pallas import tpu as pltpu
from jax.sharding import PartitionSpec as P

MESH = pl.DeviceIdType.MESH
BF = jnp.bfloat16
F32 = jnp.float32
L = 128


def sigmoid(v):
    return 0.5 * jnp.tanh(0.5 * v) + 0.5


def make_kernel(steps, tile_h, tile_w, batch, ch, n_cols):
    half_w = tile_w // 2

    def kernel(frames, h0, wx, wz, wn, bias, h_seq, h_last,
               xs, hs, ob, pm, xb, hb, rb, hf, zf, gv, wxv, wzv, wnv, send_sem, recv_sem, load_sem, out_sem):
        row = lax.axis_index('rows')
        col = lax.axis_index('cols')
        other = 1 - row
        first = (n_cols - col) // n_cols
        final = (col + 1) // n_cols
        left, right = col - 1 + first, col + 1 - final
        left_row, right_row = row + first * (1 - 2 * row), row + final * (1 - 2 * row)
        to_left, to_right = tile_w + 1 + first, final * (tile_w + 2)
        src_row = tile_h - (tile_h - 1) * row
        dst_row = (tile_h + 1) * row

        barrier = pltpu.get_barrier_semaphore()

        def greet(c, r):
            pl.semaphore_signal(barrier, inc=1, device_id={'cols': c, 'rows': r}, device_id_type=MESH)

        greet(col, other)
        greet(left, left_row)
        greet(left, other)
        greet(right, right_row)
        greet(right, other)

        inner = (pl.ds(1, tile_h), pl.ds(1, tile_w))

        def load_frame(t):
            return pltpu.make_async_copy(frames.at[t], xs.at[t], load_sem.at[t])

        def load_w(src, dst, first, width, sem):
            return pltpu.make_async_copy(src.at[:, pl.ds(first, width)], dst.at[:, pl.ds(first, width)], load_sem.at[sem])

        s0 = steps + 1
        load_h = [pltpu.make_async_copy(h0.at[:, :, pl.ds(g * L, L)], hs.at[g, :, pl.ds(0, tile_h * tile_w)], load_sem.at[s0 + 6 + g])
                  for g in range(ch // L)]
        load_xbc = load_w(wx, wxv, 256, 512, s0)
        load_xa = load_w(wx, wxv, 0, 256, s0 + 2)
        load_xd = load_w(wx, wxv, 768, 256, s0 + 1)
        load_z = load_w(wz, wzv, 0, 768, s0 + 3)
        load_xe = load_w(wx, wxv, 1024, 128, s0 + 4)
        load_n = load_w(wn, wnv, 0, 384, s0 + 5)
        load_frame(0).start()
        for cp in load_h:
            cp.start()
        load_xbc.start()
        for t in range(1, steps):
            load_frame(t).start()
        load_xa.start()
        load_z.start()
        load_xd.start()
        load_xe.start()
        load_n.start()

        def zero_border(buf, i):
            buf[i, (tile_h + 1) * row] = jnp.zeros((tile_w + 3, batch, ch), BF)

            @pl.when(first == 1)
            def _():
                buf[i, :, 0:1] = jnp.zeros((tile_h + 2, 1, batch, ch), BF)

            @pl.when(final == 1)
            def _():
                buf[i, :, tile_w + 1:tile_w + 2] = jnp.zeros((tile_h + 2, 1, batch, ch), BF)

        def zero_borders():
            @pl.loop(0, 2)
            def _(i):
                zero_border(hb, i)
                zero_border(rb, i)

            @pl.loop(0, steps)
            def _(t):
                zero_border(xb, t)

        def copies(buf, i, slot, first=first, final=final):
            def rc(src, dst, k, land, c, r):
                return pltpu.make_async_remote_copy(
                    src_ref=buf.at[(i,) + src], dst_ref=buf.at[(i,) + dst], send_sem=send_sem.at[slot, k],
                    recv_sem=recv_sem.at[slot, land], device_id={'cols': c, 'rows': r}, device_id_type=MESH)
            rows = pl.ds(1, tile_h)
            return (
                rc((src_row, pl.ds(1, tile_w)), (dst_row, pl.ds(1, tile_w)), 0, 0, col, other),
                rc((rows, 1), (rows, to_left), 1, 1 + first, left, left_row),
                rc((rows, tile_w), (rows, to_right), 2, 2 - final, right, right_row),
                rc((src_row, 1), (dst_row, to_left), 3, 3 + first, left, other),
                rc((src_row, tile_w), (dst_row, to_right), 4, 4 - final, right, other),
            )

        def send(buf, i, slot):
            for cp in copies(buf, i, slot):
                cp.start()

        def wait_rows(buf, i, slot):
            copies(buf, i, slot)[0].wait_recv()

        def wait_cols(buf, i, slot):
            for cp in copies(buf, i, slot, 0, 0)[1:]:
                cp.wait_recv()
            for cp in copies(buf, i, slot):
                cp.wait_send()

        def dot(lhs, rhs, rows, cols):
            return jnp.dot(jnp.concatenate(lhs, axis=1), jnp.concatenate(rhs, axis=0),
                           preferred_element_type=F32).reshape(rows, cols, batch, -1)

        def view(buf, i, a, rows, c, c0, c1):
            return buf[i, a:a + rows, c0 + c:c1 + c].reshape(rows * (c1 - c0) * batch, ch)

        def part(srcs, cs, c0, c1, n):
            if n > L:
                lhs, rhs = [], []
                for (buf, i, w, first) in srcs:
                    for c in cs:
                        for a in range(3):
                            lhs.append(view(buf, i, a, tile_h, c, c0, c1))
                            rhs.append(w[(a * 3 + c) * ch:(a * 3 + c + 1) * ch, first:first + n])
                return dot(lhs, rhs, tile_h, c1 - c0)
            lhs, rhs, lhs_2, rhs_2 = [], [], [], []
            both = len(cs) == 2
            low = min(cs)
            for (buf, i, w, first_n) in srcs:
                tap = {(a, c): w[(a * 3 + c) * ch:(a * 3 + c + 1) * ch, first_n:first_n + n] for c in cs for a in range(3)}
                for c in cs:
                    lhs.append(view(buf, i, 0, tile_h + 1, c, c0, c1))
                    rhs.append(jnp.concatenate([tap[0, c], tap[1, c]], axis=1))
                lhs_2.append(view(buf, i, 2, tile_h, low, c0, c1 + both))
                rhs_2.append(jnp.concatenate([tap[2, low], tap[2, low + 1]], axis=1) if both else tap[2, low])
            pair = dot(lhs, rhs, tile_h + 1, c1 - c0)
            out = pair[:tile_h, :, :, :L] + pair[1:, :, :, L:]
            pair = dot(lhs_2, rhs_2, tile_h, c1 - c0 + both)
            return out + (pair[:, :-1, :, :L] + pair[:, 1:, :, L:] if both else pair)

        halves = (((1, 2), 0, half_w), ((1, 0), half_w, tile_w))
        inner_far = (((0,), 1, half_w), ((2,), half_w, tile_w - 1))
        edge_far = (((0,), 0, 1), ((2,), tile_w - 1, tile_w))

        def slot_at(s, c0, c1, n):
            return (s, slice(None), slice(c0, c1), slice(None), slice(0, n))

        def put(s, srcs, n=256, which=halves):
            for (cs, c0, c1) in which:
                gv[slot_at(s, c0, c1, n)] = part(srcs, cs, c0, c1, n)

        def add(s, srcs, n=256, which=halves):
            for (cs, c0, c1) in which:
                idx = slot_at(s, c0, c1, n)
                gv[idx] = gv[idx] + part(srcs, cs, c0, c1, n)

        def finish(s, srcs, which, end, n=256):
            for (cs, c0, c1) in which:
                end(gv[slot_at(s, c0, c1, n)] + part(srcs, cs, c0, c1, n), c0, c1)

        pitch = tile_h * tile_w + 8

        def flat(g):
            return hs.at[g].reshape(batch * pitch, L)

        def lanes(g):
            return (slice(None), slice(g * L, (g + 1) * L))

        def at(c0, c1):
            return (slice(None), slice(c0, c1))

        def at_pad(c0, c1):
            return (slice(1, tile_h + 1), slice(1 + c0, 1 + c1))

        def b_of(first):
            return bias[first:first + L].reshape(1, 1, 1, L)

        def reset_part(v, g, c0, c1, par):
            r = sigmoid(v + b_of(ch + g * L))
            rb[(par,) + at_pad(c0, c1) + lanes(g)] = (r * hf[at(c0, c1) + lanes(g)]).astype(BF)

        def update_part(v, g, c0, c1):
            zf[at(c0, c1) + lanes(g)] = sigmoid(v + b_of(g * L))

        def state_part(v, g, c0, c1, nxt):
            idx = at(c0, c1) + lanes(g)
            n = jnp.tanh(v + b_of(2 * ch + g * L))
            z = zf[idx]
            h = (1.0 - z) * n + z * hf[idx]
            hf[idx] = h
            hb[(nxt,) + at_pad(c0, c1) + lanes(g)] = h.astype(BF)
            for r in range(tile_h):
                for c in range(c0, c1):
                    flat(g)[pl.ds(r * tile_w + c, batch, stride=pitch), :] = h[r, c - c0]

        def end_a(v, c0, c1):
            update_part(v[..., :L], 0, c0, c1)
            update_part(v[..., L:], 1, c0, c1)

        def end_b(par):
            def end(v, c0, c1):
                update_part(v[..., :L], 2, c0, c1)
                reset_part(v[..., L:], 0, c0, c1, par)
            return end

        def end_c(par):
            def end(v, c0, c1):
                reset_part(v[..., :L], 1, c0, c1, par)
                reset_part(v[..., L:], 2, c0, c1, par)
            return end

        def end_d(nxt):
            def end(v, c0, c1):
                state_part(v[..., :L], 0, c0, c1, nxt)
                state_part(v[..., L:], 1, c0, c1, nxt)
            return end

        def end_e(nxt):
            def end(v, c0, c1):
                state_part(v, 2, c0, c1, nxt)
            return end

        def permute_frame(t):
            for j in range(tile_h // 2):
                rows = [xs[t, b * tile_h * tile_w + j * 2 * tile_w:b * tile_h * tile_w + (j + 1) * 2 * tile_w] for b in range(batch)]
                out = jnp.dot(pm[...], jnp.concatenate(rows, axis=0), preferred_element_type=F32)
                xb[t, 1 + 2 * j:3 + 2 * j, 1:tile_w + 1] = out.astype(BF).reshape(2, tile_w, batch, ch)

        def make_permutation():
            n = 2 * tile_w * batch
            o = lax.broadcasted_iota(jnp.int32, (n, n), 0)
            i = lax.broadcasted_iota(jnp.int32, (n, n), 1)
            src = (o & 15) * 16 + (o >> 7) * 8 + ((o >> 4) & 7)
            pm[...] = jnp.where(i == src, 1.0, 0.0).astype(BF)

        def permute_state():
            @pl.loop(0, tile_h)
            def _(r):
                for c in range(tile_w):
                    for g in range(ch // L):
                        v = flat(g)[pl.ds(r * tile_w + c, batch, stride=pitch), :]
                        hf[r, c, :, g * L:(g + 1) * L] = v
                        hb[0, 1 + r, 1 + c, :, g * L:(g + 1) * L] = v.astype(BF)

        def round_state():
            for b in range(batch):
                for g in range(ch // L):
                    ob[b * tile_h * tile_w:(b + 1) * tile_h * tile_w, g * L:(g + 1) * L] = hs[g, b, 0:tile_h * tile_w].astype(BF)

        def store_step(t):
            return pltpu.make_async_copy(ob, h_seq.at[t], out_sem.at[0])

        h_slot, r_slot = steps, steps + 2

        make_permutation()
        zero_borders()
        load_frame(0).wait()
        permute_frame(0)
        pl.semaphore_wait(barrier, 5)
        send(xb, 0, 0)
        for cp in load_h:
            cp.wait()
        permute_state()
        send(hb, 0, h_slot)
        for t in range(1, steps):
            load_frame(t).wait()
        for t in range(1, steps):
            permute_frame(t)
        load_xbc.wait()
        wait_rows(xb, 0, 0)

        @pl.loop(0, steps)
        def _(t):
            par = lax.rem(t, 2)
            nxt = 1 - par

            put(1, [(xb, t, wxv, 256)])
            put(2, [(xb, t, wxv, 512)])
            wait_rows(hb, par, h_slot + par)

            @pl.when(t == 0)
            def _():
                load_xa.wait()
                load_z.wait()

            add(1, [(hb, par, wzv, 256)])
            add(2, [(hb, par, wzv, 512)])
            both_b = [(xb, t, wxv, 256), (hb, par, wzv, 256)]
            both_c = [(xb, t, wxv, 512), (hb, par, wzv, 512)]
            finish(1, both_b, inner_far, end_b(par))
            finish(2, both_c, inner_far, end_c(par))
            put(0, [(xb, t, wxv, 0)])
            round_state()
            wait_cols(xb, t, t)
            wait_cols(hb, par, h_slot + par)
            store = store_step(jnp.maximum(t - 1, 0))
            store.start()
            both_a = [(xb, t, wxv, 0), (hb, par, wzv, 0)]
            finish(1, both_b, edge_far, end_b(par))
            finish(2, both_c, edge_far, end_c(par))
            add(0, both_a, which=edge_far)
            send(rb, par, r_slot + par)

            @pl.when(t < steps - 1)
            def _():
                send(xb, t + 1, t + 1)

            @pl.when(t == 0)
            def _():
                load_xd.wait()
                load_xe.wait()
                load_n.wait()

            add(0, [(hb, par, wzv, 0)])
            finish(0, both_a, inner_far, end_a)
            for (_, c0, c1) in edge_far:
                end_a(gv[slot_at(0, c0, c1, 256)], c0, c1)
            put(3, [(xb, t, wxv, 768)])
            wait_rows(rb, par, r_slot + par)


            both_d = [(xb, t, wxv, 768), (rb, par, wnv, 0)]
            both_e = [(xb, t, wxv, 1024), (rb, par, wnv, 256)]
            add(3, [(rb, par, wnv, 0)])
            put(4, both_e, n=L)
            finish(3, both_d, inner_far, end_d(nxt))
            finish(4, both_e, inner_far, end_e(nxt), n=L)
            wait_cols(rb, par, r_slot + par)
            store.wait()
            finish(3, both_d, edge_far, end_d(nxt))
            finish(4, both_e, edge_far, end_e(nxt), n=L)

            @pl.when(t < steps - 1)
            def _():
                send(hb, nxt, h_slot + nxt)
                wait_rows(xb, t + 1, t + 1)

        store_last = [pltpu.make_async_copy(hs.at[g, :, pl.ds(0, tile_h * tile_w)], h_last.at[:, :, pl.ds(g * L, L)],
                                            load_sem.at[s0 + 6 + g]) for g in range(ch // L)]
        for cp in store_last:
            cp.start()
        round_state()
        store = store_step(steps - 1)
        store.start()
        for cp in store_last:
            cp.wait()
        store.wait()

    return kernel


def solution(mesh):
    n_cols = mesh.shape['cols']
    frame_spec = P(None, 'batch', 'rows', 'cols', None)
    state_spec = P('batch', 'rows', 'cols', None)

    def local_fn(frames, h_init, w_x, w_hzr, w_hn, gate_bias):
        steps, batch, tile_h, tile_w, ch = frames.shape
        pad = (tile_h + 2, tile_w + 3, batch, ch)
        tile = (tile_h, tile_w, batch, ch)
        vmem = pltpu.VMEM
        any_spec = pl.BlockSpec(memory_space=pl.ANY)
        h_seq, h_last = pl.pallas_call(
            make_kernel(steps, tile_h, tile_w, batch, ch, n_cols),
            out_shape=(jax.ShapeDtypeStruct((steps, tile_h * tile_w * batch, ch), BF),
                       jax.ShapeDtypeStruct((batch, tile_h * tile_w, ch), F32)),
            in_specs=[any_spec] * 5 + [pl.BlockSpec(memory_space=pltpu.VMEM)],
            out_specs=(any_spec, any_spec),
            scratch_shapes=[
                vmem((steps, tile_h * tile_w * batch, ch), BF), vmem((ch // L, batch, tile_h * tile_w + 8, L), F32),
                vmem((tile_h * tile_w * batch, ch), BF), vmem((2 * tile_w * batch, 2 * tile_w * batch), BF),
                vmem((steps,) + pad, BF), vmem((2,) + pad, BF), vmem((2,) + pad, BF),
                vmem(tile, F32), vmem(tile, F32),
                vmem((5,) + tile[:3] + (256,), F32),
                vmem((9 * ch, 3 * ch), BF), vmem((9 * ch, 2 * ch), BF), vmem((9 * ch, ch), BF),
                pltpu.SemaphoreType.DMA((steps + 4, 5)), pltpu.SemaphoreType.DMA((steps + 4, 5)),
                pltpu.SemaphoreType.DMA((steps + 10,)), pltpu.SemaphoreType.DMA((1,)),
            ],
            compiler_params=pltpu.CompilerParams(collective_id=0, has_side_effects=True, vmem_limit_bytes=60 * 1024 * 1024),
            name='convgru',
        )(
            frames.reshape(steps, -1, ch), h_init.reshape(batch, -1, ch),
            w_x.reshape(9 * ch, -1), w_hzr.reshape(9 * ch, -1), w_hn.reshape(9 * ch, -1), gate_bias,
        )
        return h_seq.reshape(frames.shape), h_last.reshape(h_init.shape)

    return jax.shard_map(local_fn, mesh=mesh, in_specs=(frame_spec, state_spec, P(), P(), P(), P()),
                         out_specs=(frame_spec, state_spec), check_vma=False)
```

```python
import jax
import jax.numpy as jnp
from jax import lax
from jax.experimental import pallas as pl
from jax.experimental.pallas import tpu as pltpu
from jax.sharding import PartitionSpec as P

MESH = pl.DeviceIdType.MESH
BF = jnp.bfloat16
F32 = jnp.float32
L = 128


def sigmoid(v):
    return 0.5 * jnp.tanh(0.5 * v) + 0.5


def make_kernel(steps, tile_h, tile_w, batch, ch, n_cols):
    half_w = tile_w // 2

    def kernel(frames, h0, wx, wz, wn, bias, h_seq, h_last,
               xs, hs, pm, xb, hb, rb, hf, zf, gv, wxv, wzv, wnv, send_sem, recv_sem, load_sem):
        row = lax.axis_index('rows')
        col = lax.axis_index('cols')
        other = 1 - row
        first = (n_cols - col) // n_cols
        final = (col + 1) // n_cols
        left, right = col - 1 + first, col + 1 - final
        left_row, right_row = row + first * (1 - 2 * row), row + final * (1 - 2 * row)
        to_left, to_right = tile_w + 1 + first, final * (tile_w + 2)
        src_row = tile_h - (tile_h - 1) * row
        dst_row = (tile_h + 1) * row

        barrier = pltpu.get_barrier_semaphore()

        def greet(c, r):
            pl.semaphore_signal(barrier, inc=1, device_id={'cols': c, 'rows': r}, device_id_type=MESH)

        greet(col, other)
        greet(left, left_row)
        greet(left, other)
        greet(right, right_row)
        greet(right, other)

        inner = (pl.ds(1, tile_h), pl.ds(1, tile_w))

        def load_frame(t):
            return pltpu.make_async_copy(frames.at[t], xs.at[t], load_sem.at[t])

        def load_w(src, dst, first, width, sem):
            return pltpu.make_async_copy(src.at[:, pl.ds(first, width)], dst.at[:, pl.ds(first, width)], load_sem.at[sem])

        s0 = steps + 1
        load_h = [pltpu.make_async_copy(h0.at[:, :, pl.ds(g * L, L)], hs.at[g, :, pl.ds(0, tile_h * tile_w)], load_sem.at[s0 + 6 + g])
                  for g in range(ch // L)]
        load_xbc = load_w(wx, wxv, 256, 512, s0)
        load_xa = load_w(wx, wxv, 0, 256, s0 + 2)
        load_xd = load_w(wx, wxv, 768, 256, s0 + 1)
        load_z = load_w(wz, wzv, 0, 768, s0 + 3)
        load_xe = load_w(wx, wxv, 1024, 128, s0 + 4)
        load_n = load_w(wn, wnv, 0, 384, s0 + 5)
        load_frame(0).start()
        for cp in load_h:
            cp.start()
        load_xbc.start()
        for t in range(1, steps):
            load_frame(t).start()
        load_xa.start()
        load_z.start()
        load_xd.start()
        load_xe.start()
        load_n.start()

        def zero_border(buf, i):
            buf[i, (tile_h + 1) * row] = jnp.zeros((tile_w + 3, batch, ch), BF)

            @pl.when(first == 1)
            def _():
                buf[i, :, 0:1] = jnp.zeros((tile_h + 2, 1, batch, ch), BF)

            @pl.when(final == 1)
            def _():
                buf[i, :, tile_w + 1:tile_w + 2] = jnp.zeros((tile_h + 2, 1, batch, ch), BF)

        def zero_borders():
            @pl.loop(0, 2)
            def _(i):
                zero_border(hb, i)
                zero_border(rb, i)

            @pl.loop(0, steps)
            def _(t):
                zero_border(xb, t)

        def copies(buf, i, slot, first=first, final=final):
            def rc(src, dst, k, land, c, r):
                return pltpu.make_async_remote_copy(
                    src_ref=buf.at[(i,) + src], dst_ref=buf.at[(i,) + dst], send_sem=send_sem.at[slot, k],
                    recv_sem=recv_sem.at[slot, land], device_id={'cols': c, 'rows': r}, device_id_type=MESH)
            rows = pl.ds(1, tile_h)
            return (
                rc((src_row, pl.ds(1, tile_w)), (dst_row, pl.ds(1, tile_w)), 0, 0, col, other),
                rc((rows, 1), (rows, to_left), 1, 1 + first, left, left_row),
                rc((rows, tile_w), (rows, to_right), 2, 2 - final, right, right_row),
                rc((src_row, 1), (dst_row, to_left), 3, 3 + first, left, other),
                rc((src_row, tile_w), (dst_row, to_right), 4, 4 - final, right, other),
            )

        def send(buf, i, slot):
            for cp in copies(buf, i, slot):
                cp.start()

        def wait_rows(buf, i, slot):
            copies(buf, i, slot)[0].wait_recv()

        def wait_cols(buf, i, slot):
            for cp in copies(buf, i, slot, 0, 0)[1:]:
                cp.wait_recv()
            for cp in copies(buf, i, slot):
                cp.wait_send()

        def dot(lhs, rhs, rows, cols):
            return jnp.dot(jnp.concatenate(lhs, axis=1), jnp.concatenate(rhs, axis=0),
                           preferred_element_type=F32).reshape(rows, cols, batch, -1)

        def view(buf, i, a, rows, c, c0, c1):
            return buf[i, a:a + rows, c0 + c:c1 + c].reshape(rows * (c1 - c0) * batch, ch)

        def part(srcs, cs, c0, c1, n):
            if n > L:
                lhs, rhs = [], []
                for (buf, i, w, first) in srcs:
                    for c in cs:
                        for a in range(3):
                            lhs.append(view(buf, i, a, tile_h, c, c0, c1))
                            rhs.append(w[(a * 3 + c) * ch:(a * 3 + c + 1) * ch, first:first + n])
                return dot(lhs, rhs, tile_h, c1 - c0)
            lhs, rhs, lhs_2, rhs_2 = [], [], [], []
            both = len(cs) == 2
            low = min(cs)
            for (buf, i, w, first_n) in srcs:
                tap = {(a, c): w[(a * 3 + c) * ch:(a * 3 + c + 1) * ch, first_n:first_n + n] for c in cs for a in range(3)}
                for c in cs:
                    lhs.append(view(buf, i, 0, tile_h + 1, c, c0, c1))
                    rhs.append(jnp.concatenate([tap[0, c], tap[1, c]], axis=1))
                lhs_2.append(view(buf, i, 2, tile_h, low, c0, c1 + both))
                rhs_2.append(jnp.concatenate([tap[2, low], tap[2, low + 1]], axis=1) if both else tap[2, low])
            pair = dot(lhs, rhs, tile_h + 1, c1 - c0)
            out = pair[:tile_h, :, :, :L] + pair[1:, :, :, L:]
            pair = dot(lhs_2, rhs_2, tile_h, c1 - c0 + both)
            return out + (pair[:, :-1, :, :L] + pair[:, 1:, :, L:] if both else pair)

        halves = (((1, 2), 0, half_w), ((1, 0), half_w, tile_w))
        inner_far = (((0,), 1, half_w), ((2,), half_w, tile_w - 1))
        edge_far = (((0,), 0, 1), ((2,), tile_w - 1, tile_w))

        def slot_at(s, c0, c1, n):
            return (s, slice(None), slice(c0, c1), slice(None), slice(0, n))

        def put(s, srcs, n=256, which=halves):
            for (cs, c0, c1) in which:
                gv[slot_at(s, c0, c1, n)] = part(srcs, cs, c0, c1, n)

        def add(s, srcs, n=256, which=halves):
            for (cs, c0, c1) in which:
                idx = slot_at(s, c0, c1, n)
                gv[idx] = gv[idx] + part(srcs, cs, c0, c1, n)

        def finish(s, srcs, which, end, n=256):
            for (cs, c0, c1) in which:
                end(gv[slot_at(s, c0, c1, n)] + part(srcs, cs, c0, c1, n), c0, c1)

        pitch = tile_h * tile_w + 8

        def flat(g):
            return hs.at[g].reshape(batch * pitch, L)

        def lanes(g):
            return (slice(None), slice(g * L, (g + 1) * L))

        def at(c0, c1):
            return (slice(None), slice(c0, c1))

        def at_pad(c0, c1):
            return (slice(1, tile_h + 1), slice(1 + c0, 1 + c1))

        def b_of(first):
            return bias[first:first + L].reshape(1, 1, 1, L)

        def reset_part(v, g, c0, c1, par):
            r = sigmoid(v + b_of(ch + g * L))
            rb[(par,) + at_pad(c0, c1) + lanes(g)] = (r * hf[at(c0, c1) + lanes(g)]).astype(BF)

        def update_part(v, g, c0, c1):
            zf[at(c0, c1) + lanes(g)] = sigmoid(v + b_of(g * L))

        def state_part(v, g, c0, c1, nxt):
            idx = at(c0, c1) + lanes(g)
            n = jnp.tanh(v + b_of(2 * ch + g * L))
            z = zf[idx]
            h = (1.0 - z) * n + z * hf[idx]
            hf[idx] = h
            hb[(nxt,) + at_pad(c0, c1) + lanes(g)] = h.astype(BF)
            for r in range(tile_h):
                for c in range(c0, c1):
                    flat(g)[pl.ds(r * tile_w + c, batch, stride=pitch), :] = h[r, c - c0]

        def end_a(v, c0, c1):
            update_part(v[..., :L], 0, c0, c1)
            update_part(v[..., L:], 1, c0, c1)

        def end_b(par):
            def end(v, c0, c1):
                update_part(v[..., :L], 2, c0, c1)
                reset_part(v[..., L:], 0, c0, c1, par)
            return end

        def end_c(par):
            def end(v, c0, c1):
                reset_part(v[..., :L], 1, c0, c1, par)
                reset_part(v[..., L:], 2, c0, c1, par)
            return end

        def end_d(nxt):
            def end(v, c0, c1):
                state_part(v[..., :L], 0, c0, c1, nxt)
                state_part(v[..., L:], 1, c0, c1, nxt)
            return end

        def end_e(nxt):
            def end(v, c0, c1):
                state_part(v, 2, c0, c1, nxt)
            return end

        def permute_frame(t):
            for j in range(tile_h // 2):
                rows = [xs[t, b * tile_h * tile_w + j * 2 * tile_w:b * tile_h * tile_w + (j + 1) * 2 * tile_w] for b in range(batch)]
                out = jnp.dot(pm[...], jnp.concatenate(rows, axis=0), preferred_element_type=F32)
                xb[t, 1 + 2 * j:3 + 2 * j, 1:tile_w + 1] = out.astype(BF).reshape(2, tile_w, batch, ch)

        def make_permutation():
            n = 2 * tile_w * batch
            o = lax.broadcasted_iota(jnp.int32, (n, n), 0)
            i = lax.broadcasted_iota(jnp.int32, (n, n), 1)
            src = (o & 15) * 16 + (o >> 7) * 8 + ((o >> 4) & 7)
            pm[...] = jnp.where(i == src, 1.0, 0.0).astype(BF)

        def permute_state():
            @pl.loop(0, tile_h)
            def _(r):
                for c in range(tile_w):
                    for g in range(ch // L):
                        v = flat(g)[pl.ds(r * tile_w + c, batch, stride=pitch), :]
                        hf[r, c, :, g * L:(g + 1) * L] = v
                        hb[0, 1 + r, 1 + c, :, g * L:(g + 1) * L] = v.astype(BF)

        def round_state(t):
            for b in range(batch):
                for g in range(ch // L):
                    h_seq[t, b * tile_h * tile_w:(b + 1) * tile_h * tile_w, g * L:(g + 1) * L] = hs[g, b, 0:tile_h * tile_w].astype(BF)

        h_slot, r_slot = steps, steps + 2

        make_permutation()
        zero_borders()
        load_frame(0).wait()
        permute_frame(0)
        pl.semaphore_wait(barrier, 5)
        send(xb, 0, 0)
        for cp in load_h:
            cp.wait()
        permute_state()
        send(hb, 0, h_slot)
        for t in range(1, steps):
            load_frame(t).wait()
        for t in range(1, steps):
            permute_frame(t)
        load_xbc.wait()
        wait_rows(xb, 0, 0)

        @pl.loop(0, steps)
        def _(t):
            par = lax.rem(t, 2)
            nxt = 1 - par

            put(1, [(xb, t, wxv, 256)])
            put(2, [(xb, t, wxv, 512)])
            wait_rows(hb, par, h_slot + par)

            @pl.when(t == 0)
            def _():
                load_xa.wait()
                load_z.wait()

            add(1, [(hb, par, wzv, 256)])
            add(2, [(hb, par, wzv, 512)])
            both_b = [(xb, t, wxv, 256), (hb, par, wzv, 256)]
            both_c = [(xb, t, wxv, 512), (hb, par, wzv, 512)]
            finish(1, both_b, inner_far, end_b(par))
            finish(2, both_c, inner_far, end_c(par))
            put(0, [(xb, t, wxv, 0)])
            round_state(jnp.maximum(t - 1, 0))
            wait_cols(xb, t, t)
            wait_cols(hb, par, h_slot + par)
            both_a = [(xb, t, wxv, 0), (hb, par, wzv, 0)]
            finish(1, both_b, edge_far, end_b(par))
            finish(2, both_c, edge_far, end_c(par))
            add(0, both_a, which=edge_far)
            send(rb, par, r_slot + par)

            @pl.when(t < steps - 1)
            def _():
                send(xb, t + 1, t + 1)

            @pl.when(t == 0)
            def _():
                load_xd.wait()
                load_xe.wait()
                load_n.wait()

            add(0, [(hb, par, wzv, 0)])
            finish(0, both_a, inner_far, end_a)
            for (_, c0, c1) in edge_far:
                end_a(gv[slot_at(0, c0, c1, 256)], c0, c1)
            put(3, [(xb, t, wxv, 768)])
            wait_rows(rb, par, r_slot + par)


            both_d = [(xb, t, wxv, 768), (rb, par, wnv, 0)]
            both_e = [(xb, t, wxv, 1024), (rb, par, wnv, 256)]
            add(3, [(rb, par, wnv, 0)])
            put(4, both_e, n=L)
            finish(3, both_d, inner_far, end_d(nxt))
            finish(4, both_e, inner_far, end_e(nxt), n=L)
            wait_cols(rb, par, r_slot + par)
            finish(3, both_d, edge_far, end_d(nxt))
            finish(4, both_e, edge_far, end_e(nxt), n=L)

            @pl.when(t < steps - 1)
            def _():
                send(hb, nxt, h_slot + nxt)
                wait_rows(xb, t + 1, t + 1)

        round_state(steps - 1)
        for g in range(ch // L):
            h_last[:, :, g * L:(g + 1) * L] = hs[g, :, 0:tile_h * tile_w]

    return kernel


def solution(mesh):
    n_cols = mesh.shape['cols']
    frame_spec = P(None, 'batch', 'rows', 'cols', None)
    state_spec = P('batch', 'rows', 'cols', None)

    def local_fn(frames, h_init, w_x, w_hzr, w_hn, gate_bias):
        steps, batch, tile_h, tile_w, ch = frames.shape
        pad = (tile_h + 2, tile_w + 3, batch, ch)
        tile = (tile_h, tile_w, batch, ch)
        vmem = pltpu.VMEM
        any_spec = pl.BlockSpec(memory_space=pl.ANY)
        h_seq, h_last = pl.pallas_call(
            make_kernel(steps, tile_h, tile_w, batch, ch, n_cols),
            out_shape=(vmem((steps, tile_h * tile_w * batch, ch), BF), vmem((batch, tile_h * tile_w, ch), F32)),
            in_specs=[any_spec] * 5 + [pl.BlockSpec(memory_space=pltpu.VMEM)],
            out_specs=(pl.BlockSpec(memory_space=pltpu.VMEM),) * 2,
            scratch_shapes=[
                vmem((steps, tile_h * tile_w * batch, ch), BF), vmem((ch // L, batch, tile_h * tile_w + 8, L), F32),
                vmem((2 * tile_w * batch, 2 * tile_w * batch), BF),
                vmem((steps,) + pad, BF), vmem((2,) + pad, BF), vmem((2,) + pad, BF),
                vmem(tile, F32), vmem(tile, F32),
                vmem((5,) + tile[:3] + (256,), F32),
                vmem((9 * ch, 3 * ch), BF), vmem((9 * ch, 2 * ch), BF), vmem((9 * ch, ch), BF),
                pltpu.SemaphoreType.DMA((steps + 4, 5)), pltpu.SemaphoreType.DMA((steps + 4, 5)),
                pltpu.SemaphoreType.DMA((steps + 10,)),
            ],
            compiler_params=pltpu.CompilerParams(collective_id=0, has_side_effects=True, vmem_limit_bytes=52 * 1024 * 1024),
            name='convgru',
        )(
            frames.reshape(steps, -1, ch), h_init.reshape(batch, -1, ch),
            w_x.reshape(9 * ch, -1), w_hzr.reshape(9 * ch, -1), w_hn.reshape(9 * ch, -1), gate_bias,
        )
        return h_seq.reshape(frames.shape), h_last.reshape(h_init.shape)

    return jax.shard_map(local_fn, mesh=mesh, in_specs=(frame_spec, state_spec, P(), P(), P(), P()),
                         out_specs=(frame_spec, state_spec), check_vma=False)
```

```python
import jax
import jax.numpy as jnp
from jax import lax
from jax.experimental import pallas as pl
from jax.experimental.pallas import tpu as pltpu
from jax.sharding import PartitionSpec as P

MESH = pl.DeviceIdType.MESH
BF = jnp.bfloat16
F32 = jnp.float32
L = 128


def sigmoid(v):
    return 0.5 * jnp.tanh(0.5 * v) + 0.5


def round_state(hs, seq, t):
    groups, batch, _, _ = hs.shape
    cells = seq.shape[1] // batch
    for b in range(batch):
        for g in range(groups):
            seq[t, b * cells:(b + 1) * cells, g * L:(g + 1) * L] = hs[g, b, 0:cells].astype(BF)


def write_kernel(seq, hs, h_seq, h_last, final_seq, sem):
    steps = h_seq.shape[0]
    groups, _, _, _ = hs.shape
    cells = h_last.shape[1]
    cps = [pltpu.make_async_copy(seq.at[t], h_seq.at[t], sem.at[t]) for t in range(steps - 1)]
    cps += [pltpu.make_async_copy(hs.at[g, :, pl.ds(0, cells)], h_last.at[:, :, pl.ds(g * L, L)], sem.at[steps + g]) for g in range(groups)]
    for cp in cps:
        cp.start()
    round_state(hs, final_seq, 0)
    cps.append(pltpu.make_async_copy(final_seq.at[0], h_seq.at[steps - 1], sem.at[steps - 1]))
    cps[-1].start()
    for cp in cps:
        cp.wait()


def make_kernel(steps, tile_h, tile_w, batch, ch, n_cols):
    half_w = tile_w // 2

    def kernel(frames, h0, wx, wz, wn, bias, seq, hs,
               xs, pm, xb, hb, rb, hf, zf, gv, wxv, wzv, wnv, send_sem, recv_sem, load_sem):
        row = lax.axis_index('rows')
        col = lax.axis_index('cols')
        other = 1 - row
        first = (n_cols - col) // n_cols
        final = (col + 1) // n_cols
        left, right = col - 1 + first, col + 1 - final
        left_row, right_row = row + first * (1 - 2 * row), row + final * (1 - 2 * row)
        to_left, to_right = tile_w + 1 + first, final * (tile_w + 2)
        src_row = tile_h - (tile_h - 1) * row
        dst_row = (tile_h + 1) * row

        barrier = pltpu.get_barrier_semaphore()

        def greet(c, r):
            pl.semaphore_signal(barrier, inc=1, device_id={'cols': c, 'rows': r}, device_id_type=MESH)

        greet(col, other)
        greet(left, left_row)
        greet(left, other)
        greet(right, right_row)
        greet(right, other)

        inner = (pl.ds(1, tile_h), pl.ds(1, tile_w))

        def load_frame(t):
            return pltpu.make_async_copy(frames.at[t], xs.at[t], load_sem.at[t])

        def load_w(src, dst, first, width, sem):
            return pltpu.make_async_copy(src.at[:, pl.ds(first, width)], dst.at[:, pl.ds(first, width)], load_sem.at[sem])

        s0 = steps + 1
        load_h = [pltpu.make_async_copy(h0.at[:, :, pl.ds(g * L, L)], hs.at[g, :, pl.ds(0, tile_h * tile_w)], load_sem.at[s0 + 6 + g])
                  for g in range(ch // L)]
        load_xbc = load_w(wx, wxv, 256, 512, s0)
        load_xa = load_w(wx, wxv, 0, 256, s0 + 2)
        load_xd = load_w(wx, wxv, 768, 256, s0 + 1)
        load_z = load_w(wz, wzv, 0, 768, s0 + 3)
        load_xe = load_w(wx, wxv, 1024, 128, s0 + 4)
        load_n = load_w(wn, wnv, 0, 384, s0 + 5)
        load_frame(0).start()
        for cp in load_h:
            cp.start()
        for t in range(1, steps):
            load_frame(t).start()
        for cp in (load_xbc, load_xa, load_z, load_xd, load_xe, load_n):
            cp.start()

        def zero_border(buf, i):
            buf[i, (tile_h + 1) * row] = jnp.zeros((tile_w + 3, batch, ch), BF)

            @pl.when(first == 1)
            def _():
                buf[i, :, 0:1] = jnp.zeros((tile_h + 2, 1, batch, ch), BF)

            @pl.when(final == 1)
            def _():
                buf[i, :, tile_w + 1:tile_w + 2] = jnp.zeros((tile_h + 2, 1, batch, ch), BF)

        def zero_borders():
            @pl.loop(0, 2)
            def _(i):
                zero_border(hb, i)
                zero_border(rb, i)

            @pl.loop(0, steps)
            def _(t):
                zero_border(xb, t)

        def copies(buf, i, slot, first=first, final=final):
            def rc(src, dst, k, land, c, r):
                return pltpu.make_async_remote_copy(
                    src_ref=buf.at[(i,) + src], dst_ref=buf.at[(i,) + dst], send_sem=send_sem.at[slot, k],
                    recv_sem=recv_sem.at[slot, land], device_id={'cols': c, 'rows': r}, device_id_type=MESH)
            rows = pl.ds(1, tile_h)
            return (
                rc((src_row, pl.ds(1, tile_w)), (dst_row, pl.ds(1, tile_w)), 0, 0, col, other),
                rc((rows, 1), (rows, to_left), 1, 1 + first, left, left_row),
                rc((rows, tile_w), (rows, to_right), 2, 2 - final, right, right_row),
                rc((src_row, 1), (dst_row, to_left), 3, 3 + first, left, other),
                rc((src_row, tile_w), (dst_row, to_right), 4, 4 - final, right, other),
            )

        def send(buf, i, slot):
            for cp in copies(buf, i, slot):
                cp.start()

        def wait_rows(buf, i, slot):
            copies(buf, i, slot)[0].wait_recv()

        def wait_cols(buf, i, slot):
            for cp in copies(buf, i, slot, 0, 0)[1:]:
                cp.wait_recv()
            for cp in copies(buf, i, slot):
                cp.wait_send()

        def dot(lhs, rhs, rows, cols):
            return jnp.dot(jnp.concatenate(lhs, axis=1), jnp.concatenate(rhs, axis=0),
                           preferred_element_type=F32).reshape(rows, cols, batch, -1)

        def view(buf, i, a, rows, c, c0, c1):
            return buf[i, a:a + rows, c0 + c:c1 + c].reshape(rows * (c1 - c0) * batch, ch)

        def part(srcs, cs, c0, c1, n):
            if n > L:
                lhs, rhs = [], []
                for (buf, i, w, first) in srcs:
                    for c in cs:
                        for a in range(3):
                            lhs.append(view(buf, i, a, tile_h, c, c0, c1))
                            rhs.append(w[(a * 3 + c) * ch:(a * 3 + c + 1) * ch, first:first + n])
                return dot(lhs, rhs, tile_h, c1 - c0)
            lhs, rhs, lhs_2, rhs_2 = [], [], [], []
            both = len(cs) == 2
            low = min(cs)
            for (buf, i, w, first_n) in srcs:
                tap = {(a, c): w[(a * 3 + c) * ch:(a * 3 + c + 1) * ch, first_n:first_n + n] for c in cs for a in range(3)}
                for c in cs:
                    lhs.append(view(buf, i, 0, tile_h + 1, c, c0, c1))
                    rhs.append(jnp.concatenate([tap[0, c], tap[1, c]], axis=1))
                lhs_2.append(view(buf, i, 2, tile_h, low, c0, c1 + both))
                rhs_2.append(jnp.concatenate([tap[2, low], tap[2, low + 1]], axis=1) if both else tap[2, low])
            pair = dot(lhs, rhs, tile_h + 1, c1 - c0)
            out = pair[:tile_h, :, :, :L] + pair[1:, :, :, L:]
            pair = dot(lhs_2, rhs_2, tile_h, c1 - c0 + both)
            return out + (pair[:, :-1, :, :L] + pair[:, 1:, :, L:] if both else pair)

        halves = (((1, 2), 0, half_w), ((1, 0), half_w, tile_w))
        inner_far = (((0,), 1, half_w), ((2,), half_w, tile_w - 1))
        edge_far = (((0,), 0, 1), ((2,), tile_w - 1, tile_w))

        def slot_at(s, c0, c1, n):
            return (s, slice(None), slice(c0, c1), slice(None), slice(0, n))

        def put(s, srcs, n=256, which=halves):
            for (cs, c0, c1) in which:
                gv[slot_at(s, c0, c1, n)] = part(srcs, cs, c0, c1, n)

        def add(s, srcs, n=256, which=halves):
            for (cs, c0, c1) in which:
                idx = slot_at(s, c0, c1, n)
                gv[idx] = gv[idx] + part(srcs, cs, c0, c1, n)

        def finish(s, srcs, which, end, n=256):
            for (cs, c0, c1) in which:
                end(gv[slot_at(s, c0, c1, n)] + part(srcs, cs, c0, c1, n), c0, c1)

        pitch = tile_h * tile_w + 8

        def flat(g):
            return hs.at[g].reshape(batch * pitch, L)

        def lanes(g):
            return (slice(None), slice(g * L, (g + 1) * L))

        def at(c0, c1):
            return (slice(None), slice(c0, c1))

        def at_pad(c0, c1):
            return (slice(1, tile_h + 1), slice(1 + c0, 1 + c1))

        def b_of(first):
            return bias[first:first + L].reshape(1, 1, 1, L)

        def reset_part(v, g, c0, c1, par):
            r = sigmoid(v + b_of(ch + g * L))
            rb[(par,) + at_pad(c0, c1) + lanes(g)] = (r * hf[at(c0, c1) + lanes(g)]).astype(BF)

        def update_part(v, g, c0, c1):
            zf[at(c0, c1) + lanes(g)] = sigmoid(v + b_of(g * L))

        def state_part(v, g, c0, c1, nxt):
            idx = at(c0, c1) + lanes(g)
            n = jnp.tanh(v + b_of(2 * ch + g * L))
            z = zf[idx]
            h = (1.0 - z) * n + z * hf[idx]
            hf[idx] = h
            hb[(nxt,) + at_pad(c0, c1) + lanes(g)] = h.astype(BF)
            for r in range(tile_h):
                for c in range(c0, c1):
                    flat(g)[pl.ds(r * tile_w + c, batch, stride=pitch), :] = h[r, c - c0]

        def end_a(v, c0, c1):
            update_part(v[..., :L], 0, c0, c1)
            update_part(v[..., L:], 1, c0, c1)

        def end_b(par):
            def end(v, c0, c1):
                update_part(v[..., :L], 2, c0, c1)
                reset_part(v[..., L:], 0, c0, c1, par)
            return end

        def end_c(par):
            def end(v, c0, c1):
                reset_part(v[..., :L], 1, c0, c1, par)
                reset_part(v[..., L:], 2, c0, c1, par)
            return end

        def end_d(nxt):
            def end(v, c0, c1):
                state_part(v[..., :L], 0, c0, c1, nxt)
                state_part(v[..., L:], 1, c0, c1, nxt)
            return end

        def end_e(nxt):
            def end(v, c0, c1):
                state_part(v, 2, c0, c1, nxt)
            return end

        def permute_frame(t):
            for j in range(tile_h // 2):
                rows = [xs[t, b * tile_h * tile_w + j * 2 * tile_w:b * tile_h * tile_w + (j + 1) * 2 * tile_w] for b in range(batch)]
                out = jnp.dot(pm[...], jnp.concatenate(rows, axis=0), preferred_element_type=F32)
                xb[t, 1 + 2 * j:3 + 2 * j, 1:tile_w + 1] = out.astype(BF).reshape(2, tile_w, batch, ch)

        def make_permutation():
            n = 2 * tile_w * batch
            o = lax.broadcasted_iota(jnp.int32, (n, n), 0)
            i = lax.broadcasted_iota(jnp.int32, (n, n), 1)
            src = (o & 15) * 16 + (o >> 7) * 8 + ((o >> 4) & 7)
            pm[...] = jnp.where(i == src, 1.0, 0.0).astype(BF)

        def permute_state():
            @pl.loop(0, tile_h)
            def _(r):
                for c in range(tile_w):
                    for g in range(ch // L):
                        v = flat(g)[pl.ds(r * tile_w + c, batch, stride=pitch), :]
                        hf[r, c, :, g * L:(g + 1) * L] = v
                        hb[0, 1 + r, 1 + c, :, g * L:(g + 1) * L] = v.astype(BF)

        h_slot, r_slot = steps, steps + 2

        make_permutation()
        zero_borders()
        load_frame(0).wait()
        permute_frame(0)
        pl.semaphore_wait(barrier, 5)
        send(xb, 0, 0)
        for cp in load_h:
            cp.wait()
        permute_state()
        send(hb, 0, h_slot)
        for t in range(1, steps):
            load_frame(t).wait()
        for t in range(1, steps):
            permute_frame(t)
        load_xbc.wait()
        wait_rows(xb, 0, 0)

        @pl.loop(0, steps)
        def _(t):
            par = lax.rem(t, 2)
            nxt = 1 - par

            put(1, [(xb, t, wxv, 256)])
            put(2, [(xb, t, wxv, 512)])
            wait_rows(hb, par, h_slot + par)

            @pl.when(t == 0)
            def _():
                load_xa.wait()
                load_z.wait()

            add(1, [(hb, par, wzv, 256)])
            add(2, [(hb, par, wzv, 512)])
            both_b = [(xb, t, wxv, 256), (hb, par, wzv, 256)]
            both_c = [(xb, t, wxv, 512), (hb, par, wzv, 512)]
            finish(1, both_b, inner_far, end_b(par))
            finish(2, both_c, inner_far, end_c(par))
            put(0, [(xb, t, wxv, 0)])
            round_state(hs, seq, jnp.maximum(t - 1, 0))
            wait_cols(xb, t, t)
            wait_cols(hb, par, h_slot + par)
            both_a = [(xb, t, wxv, 0), (hb, par, wzv, 0)]
            finish(1, both_b, edge_far, end_b(par))
            finish(2, both_c, edge_far, end_c(par))
            add(0, both_a, which=edge_far)
            send(rb, par, r_slot + par)

            @pl.when(t < steps - 1)
            def _():
                send(xb, t + 1, t + 1)

            @pl.when(t == 0)
            def _():
                load_xd.wait()
                load_xe.wait()
                load_n.wait()

            add(0, [(hb, par, wzv, 0)])
            finish(0, both_a, inner_far, end_a)
            for (_, c0, c1) in edge_far:
                end_a(gv[slot_at(0, c0, c1, 256)], c0, c1)
            put(3, [(xb, t, wxv, 768)])
            wait_rows(rb, par, r_slot + par)


            both_d = [(xb, t, wxv, 768), (rb, par, wnv, 0)]
            both_e = [(xb, t, wxv, 1024), (rb, par, wnv, 256)]
            add(3, [(rb, par, wnv, 0)])
            put(4, both_e, n=L)
            finish(3, both_d, inner_far, end_d(nxt))
            finish(4, both_e, inner_far, end_e(nxt), n=L)
            wait_cols(rb, par, r_slot + par)
            finish(3, both_d, edge_far, end_d(nxt))
            finish(4, both_e, edge_far, end_e(nxt), n=L)

            @pl.when(t < steps - 1)
            def _():
                send(hb, nxt, h_slot + nxt)
                wait_rows(xb, t + 1, t + 1)

    return kernel


def solution(mesh):
    n_cols = mesh.shape['cols']
    frame_spec = P(None, 'batch', 'rows', 'cols', None)
    state_spec = P('batch', 'rows', 'cols', None)

    def local_fn(frames, h_init, w_x, w_hzr, w_hn, gate_bias):
        steps, batch, tile_h, tile_w, ch = frames.shape
        pad = (tile_h + 2, tile_w + 3, batch, ch)
        tile = (tile_h, tile_w, batch, ch)
        vmem = pltpu.VMEM
        cells = tile_h * tile_w
        any_spec = pl.BlockSpec(memory_space=pl.ANY)
        seq, staged = pl.pallas_call(
            make_kernel(steps, tile_h, tile_w, batch, ch, n_cols),
            out_shape=(vmem((steps - 1, cells * batch, ch), BF), vmem((ch // L, batch, cells + 8, L), F32)),
            in_specs=[any_spec] * 5 + [pl.BlockSpec(memory_space=pltpu.VMEM)],
            out_specs=(pl.BlockSpec(memory_space=pltpu.VMEM),) * 2,
            scratch_shapes=[
                vmem((steps, cells * batch, ch), BF),
                vmem((2 * tile_w * batch, 2 * tile_w * batch), BF),
                vmem((steps,) + pad, BF), vmem((2,) + pad, BF), vmem((2,) + pad, BF),
                vmem(tile, F32), vmem(tile, F32),
                vmem((5,) + tile[:3] + (256,), F32),
                vmem((9 * ch, 3 * ch), BF), vmem((9 * ch, 2 * ch), BF), vmem((9 * ch, ch), BF),
                pltpu.SemaphoreType.DMA((steps + 4, 5)), pltpu.SemaphoreType.DMA((steps + 4, 5)),
                pltpu.SemaphoreType.DMA((steps + 10,)),
            ],
            compiler_params=pltpu.CompilerParams(collective_id=0, has_side_effects=True, vmem_limit_bytes=52 * 1024 * 1024),
            name='convgru',
        )(
            frames.reshape(steps, -1, ch), h_init.reshape(batch, -1, ch),
            w_x.reshape(9 * ch, -1), w_hzr.reshape(9 * ch, -1), w_hn.reshape(9 * ch, -1), gate_bias,
        )
        h_seq, h_last = pl.pallas_call(
            write_kernel,
            out_shape=(jax.ShapeDtypeStruct((steps, cells * batch, ch), BF), jax.ShapeDtypeStruct((batch, cells, ch), F32)),
            in_specs=[pl.BlockSpec(memory_space=pltpu.VMEM)] * 2,
            out_specs=(any_spec, any_spec),
            scratch_shapes=[vmem((1, cells * batch, ch), BF), pltpu.SemaphoreType.DMA((steps + ch // L,))],
            compiler_params=pltpu.CompilerParams(vmem_limit_bytes=8 * 1024 * 1024),
            name='write_out',
        )(seq, staged)
        return h_seq.reshape(frames.shape), h_last.reshape(h_init.shape)

    return jax.shard_map(local_fn, mesh=mesh, in_specs=(frame_spec, state_spec, P(), P(), P(), P()),
                         out_specs=(frame_spec, state_spec), check_vma=False)
```

```python
import jax
import jax.numpy as jnp
from jax import lax
from jax.experimental import pallas as pl
from jax.experimental.pallas import tpu as pltpu
from jax.sharding import PartitionSpec as P

MESH = pl.DeviceIdType.MESH
BF = jnp.bfloat16
F32 = jnp.float32
L = 128


def sigmoid(v):
    return 0.5 * jnp.tanh(0.5 * v) + 0.5


def round_state(hs, seq, t):
    groups, batch, _, _ = hs.shape
    cells = seq.shape[1] // batch
    for b in range(batch):
        for g in range(groups):
            seq[t, b * cells:(b + 1) * cells, g * L:(g + 1) * L] = hs[g, b, 0:cells].astype(BF)


def write_kernel(seq, hs, h_seq, h_last, final_seq, sem):
    steps = h_seq.shape[0]
    groups, _, _, _ = hs.shape
    cells = h_last.shape[1]
    cps = [pltpu.make_async_copy(seq.at[t], h_seq.at[t], sem.at[t]) for t in range(steps - 1)]
    cps += [pltpu.make_async_copy(hs.at[g, :, pl.ds(0, cells)], h_last.at[:, :, pl.ds(g * L, L)], sem.at[steps + g]) for g in range(groups)]
    for cp in cps:
        cp.start()
    round_state(hs, final_seq, 0)
    cps.append(pltpu.make_async_copy(final_seq.at[0], h_seq.at[steps - 1], sem.at[steps - 1]))
    cps[-1].start()
    for cp in cps:
        cp.wait()


def make_kernel(steps, tile_h, tile_w, batch, ch, n_cols):
    half_w = tile_w // 2

    def kernel(frames, h0, wx, wz, wn, bias, seq, hs,
               xs, pm, xb, hb, rb, hf, zf, gv, wxv, wzv, wnv, send_sem, recv_sem, load_sem):
        row = lax.axis_index('rows')
        col = lax.axis_index('cols')
        other = 1 - row
        first = (n_cols - col) // n_cols
        final = (col + 1) // n_cols
        left, right = col - 1 + first, col + 1 - final
        left_row, right_row = row + first * (1 - 2 * row), row + final * (1 - 2 * row)
        to_left, to_right = tile_w + 1 + first, final * (tile_w + 2)
        src_row = tile_h - (tile_h - 1) * row
        dst_row = (tile_h + 1) * row

        barrier = pltpu.get_barrier_semaphore()

        def greet(c, r):
            pl.semaphore_signal(barrier, inc=1, device_id={'cols': c, 'rows': r}, device_id_type=MESH)

        greet(col, other)
        greet(left, left_row)
        greet(left, other)
        greet(right, right_row)
        greet(right, other)

        inner = (pl.ds(1, tile_h), pl.ds(1, tile_w))

        def load_frame(t):
            return pltpu.make_async_copy(frames.at[t], xs.at[t], load_sem.at[t])

        def load_w(src, dst, first, width, sem):
            return pltpu.make_async_copy(src.at[:, pl.ds(first, width)], dst.at[:, pl.ds(first, width)], load_sem.at[sem])

        s0 = steps + 1
        load_h = [pltpu.make_async_copy(h0.at[:, :, pl.ds(g * L, L)], hs.at[g, :, pl.ds(0, tile_h * tile_w)], load_sem.at[s0 + 6 + g])
                  for g in range(ch // L)]
        load_xbc = load_w(wx, wxv, 256, 512, s0)
        load_xa = load_w(wx, wxv, 0, 256, s0 + 2)
        load_xd = load_w(wx, wxv, 768, 256, s0 + 1)
        load_z = load_w(wz, wzv, 0, 768, s0 + 3)
        load_xe = load_w(wx, wxv, 1024, 128, s0 + 4)
        load_n = load_w(wn, wnv, 0, 384, s0 + 5)
        load_frame(0).start()
        for cp in load_h:
            cp.start()
        for t in range(1, steps):
            load_frame(t).start()
        for cp in (load_xbc, load_xa, load_z, load_xd, load_xe, load_n):
            cp.start()

        def zero_border(buf, i):
            buf[i, (tile_h + 1) * row] = jnp.zeros((tile_w + 3, batch, ch), BF)

            @pl.when(first == 1)
            def _():
                buf[i, :, 0:1] = jnp.zeros((tile_h + 2, 1, batch, ch), BF)

            @pl.when(final == 1)
            def _():
                buf[i, :, tile_w + 1:tile_w + 2] = jnp.zeros((tile_h + 2, 1, batch, ch), BF)

        def zero_borders():
            @pl.loop(0, 2)
            def _(i):
                zero_border(hb, i)
                zero_border(rb, i)

            @pl.loop(0, steps)
            def _(t):
                zero_border(xb, t)

        def copies(buf, i, slot, first=first, final=final):
            def rc(src, dst, k, land, c, r):
                return pltpu.make_async_remote_copy(
                    src_ref=buf.at[(i,) + src], dst_ref=buf.at[(i,) + dst], send_sem=send_sem.at[slot, k],
                    recv_sem=recv_sem.at[slot, land], device_id={'cols': c, 'rows': r}, device_id_type=MESH)
            rows = pl.ds(1, tile_h)
            return (
                rc((src_row, pl.ds(1, tile_w)), (dst_row, pl.ds(1, tile_w)), 0, 0, col, other),
                rc((rows, 1), (rows, to_left), 1, 1 + first, left, left_row),
                rc((rows, tile_w), (rows, to_right), 2, 2 - final, right, right_row),
                rc((src_row, 1), (dst_row, to_left), 3, 3 + first, left, other),
                rc((src_row, tile_w), (dst_row, to_right), 4, 4 - final, right, other),
            )

        def send(buf, i, slot):
            for cp in copies(buf, i, slot):
                cp.start()

        def wait_rows(buf, i, slot):
            copies(buf, i, slot)[0].wait_recv()

        def wait_cols(buf, i, slot):
            for cp in copies(buf, i, slot, 0, 0)[1:]:
                cp.wait_recv()
            for cp in copies(buf, i, slot):
                cp.wait_send()

        def dot(lhs, rhs, rows, cols):
            return jnp.dot(jnp.concatenate(lhs, axis=1), jnp.concatenate(rhs, axis=0),
                           preferred_element_type=F32).reshape(rows, cols, batch, -1)

        def view(buf, i, a, rows, c, c0, c1):
            return buf[i, a:a + rows, c0 + c:c1 + c].reshape(rows * (c1 - c0) * batch, ch)

        def part(srcs, cs, c0, c1, n):
            if n > L:
                lhs, rhs = [], []
                for (buf, i, w, first) in srcs:
                    for c in cs:
                        for a in range(3):
                            lhs.append(view(buf, i, a, tile_h, c, c0, c1))
                            rhs.append(w[(a * 3 + c) * ch:(a * 3 + c + 1) * ch, first:first + n])
                return dot(lhs, rhs, tile_h, c1 - c0)
            lhs, rhs, lhs_2, rhs_2 = [], [], [], []
            both = len(cs) == 2
            low = min(cs)
            for (buf, i, w, first_n) in srcs:
                tap = {(a, c): w[(a * 3 + c) * ch:(a * 3 + c + 1) * ch, first_n:first_n + n] for c in cs for a in range(3)}
                for c in cs:
                    lhs.append(view(buf, i, 0, tile_h + 1, c, c0, c1))
                    rhs.append(jnp.concatenate([tap[0, c], tap[1, c]], axis=1))
                lhs_2.append(view(buf, i, 2, tile_h, low, c0, c1 + both))
                rhs_2.append(jnp.concatenate([tap[2, low], tap[2, low + 1]], axis=1) if both else tap[2, low])
            pair = dot(lhs, rhs, tile_h + 1, c1 - c0)
            out = pair[:tile_h, :, :, :L] + pair[1:, :, :, L:]
            pair = dot(lhs_2, rhs_2, tile_h, c1 - c0 + both)
            return out + (pair[:, :-1, :, :L] + pair[:, 1:, :, L:] if both else pair)

        halves = (((1, 2), 0, half_w), ((1, 0), half_w, tile_w))
        inner_far = (((0,), 1, half_w), ((2,), half_w, tile_w - 1))
        edge_far = (((0,), 0, 1), ((2,), tile_w - 1, tile_w))

        def slot_at(s, c0, c1, n):
            return (s, slice(None), slice(c0, c1), slice(None), slice(0, n))

        def put(s, srcs, n=256, which=halves):
            for (cs, c0, c1) in which:
                gv[slot_at(s, c0, c1, n)] = part(srcs, cs, c0, c1, n)

        def add(s, srcs, n=256, which=halves):
            for (cs, c0, c1) in which:
                idx = slot_at(s, c0, c1, n)
                gv[idx] = gv[idx] + part(srcs, cs, c0, c1, n)

        def finish(s, srcs, which, end, n=256):
            for (cs, c0, c1) in which:
                end(gv[slot_at(s, c0, c1, n)] + part(srcs, cs, c0, c1, n), c0, c1)

        pitch = tile_h * tile_w + 8

        def flat(g):
            return hs.at[g].reshape(batch * pitch, L)

        def lanes(g):
            return (slice(None), slice(g * L, (g + 1) * L))

        def at(c0, c1):
            return (slice(None), slice(c0, c1))

        def at_pad(c0, c1):
            return (slice(1, tile_h + 1), slice(1 + c0, 1 + c1))

        def b_of(first):
            return bias[first:first + L].reshape(1, 1, 1, L)

        def reset_part(v, g, c0, c1, par):
            r = sigmoid(v + b_of(ch + g * L))
            rb[(par,) + at_pad(c0, c1) + lanes(g)] = (r * hf[at(c0, c1) + lanes(g)]).astype(BF)

        def update_part(v, g, c0, c1):
            zf[at(c0, c1) + lanes(g)] = sigmoid(v + b_of(g * L))

        def state_part(v, g, c0, c1, nxt):
            idx = at(c0, c1) + lanes(g)
            n = jnp.tanh(v + b_of(2 * ch + g * L))
            z = zf[idx]
            h = (1.0 - z) * n + z * hf[idx]
            hf[idx] = h
            hb[(nxt,) + at_pad(c0, c1) + lanes(g)] = h.astype(BF)
            for r in range(tile_h):
                for c in range(c0, c1):
                    flat(g)[pl.ds(r * tile_w + c, batch, stride=pitch), :] = h[r, c - c0]

        def end_a(v, c0, c1):
            update_part(v[..., :L], 0, c0, c1)
            update_part(v[..., L:], 1, c0, c1)

        def end_b(par):
            def end(v, c0, c1):
                update_part(v[..., :L], 2, c0, c1)
                reset_part(v[..., L:], 0, c0, c1, par)
            return end

        def end_c(par):
            def end(v, c0, c1):
                reset_part(v[..., :L], 1, c0, c1, par)
                reset_part(v[..., L:], 2, c0, c1, par)
            return end

        def end_d(nxt):
            def end(v, c0, c1):
                state_part(v[..., :L], 0, c0, c1, nxt)
                state_part(v[..., L:], 1, c0, c1, nxt)
            return end

        def end_e(nxt):
            def end(v, c0, c1):
                state_part(v, 2, c0, c1, nxt)
            return end

        def permute_frame(t):
            for j in range(tile_h // 2):
                rows = [xs[t, b * tile_h * tile_w + j * 2 * tile_w:b * tile_h * tile_w + (j + 1) * 2 * tile_w] for b in range(batch)]
                out = jnp.dot(pm[...], jnp.concatenate(rows, axis=0), preferred_element_type=F32)
                xb[t, 1 + 2 * j:3 + 2 * j, 1:tile_w + 1] = out.astype(BF).reshape(2, tile_w, batch, ch)

        def make_permutation():
            n = 2 * tile_w * batch
            o = lax.broadcasted_iota(jnp.int32, (n, n), 0)
            i = lax.broadcasted_iota(jnp.int32, (n, n), 1)
            src = (o & 15) * 16 + (o >> 7) * 8 + ((o >> 4) & 7)
            pm[...] = jnp.where(i == src, 1.0, 0.0).astype(BF)

        def permute_state():
            @pl.loop(0, tile_h)
            def _(r):
                for c in range(tile_w):
                    for g in range(ch // L):
                        v = flat(g)[pl.ds(r * tile_w + c, batch, stride=pitch), :]
                        hf[r, c, :, g * L:(g + 1) * L] = v
                        hb[0, 1 + r, 1 + c, :, g * L:(g + 1) * L] = v.astype(BF)

        h_slot, r_slot = steps, steps + 2

        make_permutation()
        zero_borders()
        load_frame(0).wait()
        permute_frame(0)
        pl.semaphore_wait(barrier, 5)
        send(xb, 0, 0)
        for cp in load_h:
            cp.wait()
        permute_state()
        send(hb, 0, h_slot)
        for t in range(1, steps):
            load_frame(t).wait()
        for t in range(1, steps):
            permute_frame(t)
        load_xbc.wait()
        wait_rows(xb, 0, 0)

        @pl.loop(0, steps)
        def _(t):
            par = lax.rem(t, 2)
            nxt = 1 - par

            put(1, [(xb, t, wxv, 256)])
            put(2, [(xb, t, wxv, 512)])
            wait_rows(hb, par, h_slot + par)

            @pl.when(t == 0)
            def _():
                load_xa.wait()
                load_z.wait()

            add(1, [(hb, par, wzv, 256)])
            add(2, [(hb, par, wzv, 512)])
            both_b = [(xb, t, wxv, 256), (hb, par, wzv, 256)]
            both_c = [(xb, t, wxv, 512), (hb, par, wzv, 512)]
            finish(1, both_b, inner_far, end_b(par))
            finish(2, both_c, inner_far, end_c(par))
            put(0, [(xb, t, wxv, 0)])
            round_state(hs, seq, jnp.maximum(t - 1, 0))
            wait_cols(xb, t, t)
            add(1, [(xb, t, wxv, 256)], which=edge_far)
            add(2, [(xb, t, wxv, 512)], which=edge_far)
            wait_cols(hb, par, h_slot + par)
            both_a = [(xb, t, wxv, 0), (hb, par, wzv, 0)]
            finish(1, [(hb, par, wzv, 256)], edge_far, end_b(par))
            finish(2, [(hb, par, wzv, 512)], edge_far, end_c(par))
            add(0, [(hb, par, wzv, 0)], which=edge_far)
            send(rb, par, r_slot + par)

            @pl.when(t < steps - 1)
            def _():
                send(xb, t + 1, t + 1)

            @pl.when(t == 0)
            def _():
                load_xd.wait()
                load_xe.wait()
                load_n.wait()

            add(0, [(hb, par, wzv, 0)])
            finish(0, both_a, inner_far, end_a)
            finish(0, [(xb, t, wxv, 0)], edge_far, end_a)
            put(3, [(xb, t, wxv, 768)])
            wait_rows(rb, par, r_slot + par)


            both_d = [(xb, t, wxv, 768), (rb, par, wnv, 0)]
            both_e = [(xb, t, wxv, 1024), (rb, par, wnv, 256)]
            add(3, [(rb, par, wnv, 0)])
            put(4, both_e, n=L)
            finish(3, both_d, inner_far, end_d(nxt))
            finish(4, both_e, inner_far, end_e(nxt), n=L)
            add(3, [(xb, t, wxv, 768)], which=edge_far)
            add(4, [(xb, t, wxv, 1024)], n=L, which=edge_far)
            wait_cols(rb, par, r_slot + par)
            finish(3, [(rb, par, wnv, 0)], edge_far, end_d(nxt))
            finish(4, [(rb, par, wnv, 256)], edge_far, end_e(nxt), n=L)

            @pl.when(t < steps - 1)
            def _():
                send(hb, nxt, h_slot + nxt)
                wait_rows(xb, t + 1, t + 1)

    return kernel


def solution(mesh):
    n_cols = mesh.shape['cols']
    frame_spec = P(None, 'batch', 'rows', 'cols', None)
    state_spec = P('batch', 'rows', 'cols', None)

    def local_fn(frames, h_init, w_x, w_hzr, w_hn, gate_bias):
        steps, batch, tile_h, tile_w, ch = frames.shape
        pad = (tile_h + 2, tile_w + 3, batch, ch)
        tile = (tile_h, tile_w, batch, ch)
        vmem = pltpu.VMEM
        cells = tile_h * tile_w
        any_spec = pl.BlockSpec(memory_space=pl.ANY)
        seq, staged = pl.pallas_call(
            make_kernel(steps, tile_h, tile_w, batch, ch, n_cols),
            out_shape=(vmem((steps - 1, cells * batch, ch), BF), vmem((ch // L, batch, cells + 8, L), F32)),
            in_specs=[any_spec] * 5 + [pl.BlockSpec(memory_space=pltpu.VMEM)],
            out_specs=(pl.BlockSpec(memory_space=pltpu.VMEM),) * 2,
            scratch_shapes=[
                vmem((steps, cells * batch, ch), BF),
                vmem((2 * tile_w * batch, 2 * tile_w * batch), BF),
                vmem((steps,) + pad, BF), vmem((2,) + pad, BF), vmem((2,) + pad, BF),
                vmem(tile, F32), vmem(tile, F32),
                vmem((5,) + tile[:3] + (256,), F32),
                vmem((9 * ch, 3 * ch), BF), vmem((9 * ch, 2 * ch), BF), vmem((9 * ch, ch), BF),
                pltpu.SemaphoreType.DMA((steps + 4, 5)), pltpu.SemaphoreType.DMA((steps + 4, 5)),
                pltpu.SemaphoreType.DMA((steps + 10,)),
            ],
            compiler_params=pltpu.CompilerParams(collective_id=0, has_side_effects=True, vmem_limit_bytes=52 * 1024 * 1024),
            name='convgru',
        )(
            frames.reshape(steps, -1, ch), h_init.reshape(batch, -1, ch),
            w_x.reshape(9 * ch, -1), w_hzr.reshape(9 * ch, -1), w_hn.reshape(9 * ch, -1), gate_bias,
        )
        h_seq, h_last = pl.pallas_call(
            write_kernel,
            out_shape=(jax.ShapeDtypeStruct((steps, cells * batch, ch), BF), jax.ShapeDtypeStruct((batch, cells, ch), F32)),
            in_specs=[pl.BlockSpec(memory_space=pltpu.VMEM)] * 2,
            out_specs=(any_spec, any_spec),
            scratch_shapes=[vmem((1, cells * batch, ch), BF), pltpu.SemaphoreType.DMA((steps + ch // L,))],
            compiler_params=pltpu.CompilerParams(vmem_limit_bytes=8 * 1024 * 1024),
            name='write_out',
        )(seq, staged)
        return h_seq.reshape(frames.shape), h_last.reshape(h_init.shape)

    return jax.shard_map(local_fn, mesh=mesh, in_specs=(frame_spec, state_spec, P(), P(), P(), P()),
                         out_specs=(frame_spec, state_spec), check_vma=False)
```
